128 devices in a mesh: dp: 32 (over x, z, core), tp: 4 (over y).
Axes of the slice: x: 4, y: 4, z: 4, core: 2. Of those that a mesh axis runs over, the one named last changes fastest.
Arguments:
- hidden_in: bfloat16 [2048, 3584], P(('dp', 'tp')), may hold values from -6 to 6
- query_latent: bfloat16 [2048, 64, 512], P(('dp', 'tp')), may hold values from -348 to 347
- query_rope: bfloat16 [2048, 4096], P(('dp', 'tp')), may hold values from -348 to 347
- cache_latent: bfloat16 [2048, 128, 512], P(('dp', 'tp')), may hold values from -6 to 6
- cache_rope: bfloat16 [2048, 64, 128], P(('dp', 'tp')), may hold values from -6 to 6
- lengths: int32 [2048], P(('dp', 'tp')), may hold values from 16 to 128
- value_up: bfloat16 [512, 4096], P(None, 'tp'), may hold values from -1 to 1
- out_proj: bfloat16 [4096, 3584], P('tp'), may hold values from -0.09375 to 0.09375
- norm_gain: float32 [3584], replicated, may hold values from 0.1 to 1.9
- expert_gate: bfloat16 [128, 3584, 1024], P(('dp', 'tp')), may hold values from -0.09375 to 0.09375
- expert_down: bfloat16 [128, 1024, 3584], P(('dp', 'tp')), may hold values from -0.1875 to 0.1875
- expert_ids: int32 [2048, 8], P(('dp', 'tp')), may hold values from 0 to 127, all different within a row; in each aligned block of 16 rows (0 to 15, 16 to 31, ...) at most 2 rows name the same one
- affinity: float32 [2048, 8], P(('dp', 'tp')), may hold values from 0.05 to 1
Outputs:
- layer_out: bfloat16 [2048, 3584], P(('dp', 'tp'))
The draws below stay inside these ranges and needn't reach their ends.
Inputs may be any that keep to these rules, and one draw needn't show every extreme that they name: `expert_ids`: in each aligned block of 16 rows (the rows of one device) no expert is named by more than 2 rows.
All inputs are finite; a program needn't handle non-finite values.
Results may differ from the reference program's by a relative error of at most 0.0081.
Values may be sent and summed in bfloat16 or wider, within the bound.
A program may use at most 128 MiB of HBM per device.

```python
import math
import jax
import jax.numpy as jnp
import numpy as np
from jax import lax

D = 3584
HEADS = 64
LAT = 512
ROPE = 64
HEAD_V = 64
FF = 1024
TOPK = 8
CTX = 128
TOK_DEV = 16
TOKENS = 2048
EXPERTS = 128
CAP = 2


def key_parts(key):
    latent = jax.random.normal(jax.random.fold_in(key, 101), (TOKENS, CTX, LAT), jnp.float32)
    rotary = jax.random.normal(jax.random.fold_in(key, 102), (TOKENS, ROPE, CTX), jnp.float32)
    latent = jnp.clip(latent, -6.0, 6.0).astype(jnp.bfloat16).astype(jnp.float32)
    rotary = jnp.clip(rotary, -6.0, 6.0).astype(jnp.bfloat16).astype(jnp.float32)
    return (latent, rotary)


def draw_cache_latent(key, part):
    return key_parts(key)[0].astype(jnp.bfloat16)


def draw_cache_rope(key, part):
    return key_parts(key)[1].astype(jnp.bfloat16)


def query_parts(key):
    full_shape = (TOKENS, HEADS, LAT + ROPE)
    return jnp.clip(jax.random.normal(jax.random.fold_in(key, 103), full_shape, jnp.float32), -6.0, 6.0)


def draw_query_latent(key, part):
    return query_parts(key)[:, :, :LAT].astype(jnp.bfloat16)


def draw_query_rope(key, part):
    return query_parts(key)[:, :, LAT:].reshape(TOKENS, HEADS * ROPE).astype(jnp.bfloat16)


def plant(result, rng, smallest, high):
    spot = [jax.random.randint(jax.random.fold_in(rng, axis), (), 0, length) for axis, length in enumerate(result.shape)]
    main_axis = result.shape.index(max(result.shape))
    beside = spot[:main_axis] + [(spot[main_axis] + 1) % result.shape[main_axis]] + spot[main_axis + 1:]
    return result.at[tuple(spot)].set(smallest).at[tuple(beside)].set(high)


def shard_levels(own_key, extent, pieces, smallest, top_value):
    def one(axis_at, shards_of):
        draws = jax.random.uniform(jax.random.fold_in(jax.random.fold_in(own_key, 6), axis_at), (shards_of,), jnp.float32, smallest / len(pieces), top_value / len(pieces))
        return jnp.repeat(jnp.exp(draws), extent[axis_at] // shards_of).reshape((-1,) + (1,) * (len(extent) - axis_at - 1))

    level = one(*pieces[0])
    for cut in pieces[1:]:
        level = level * one(*cut)
    return level


def shared_out(key, own, number, rows, number_of, top, limit, slope):
    sequence = jax.random.permutation(key, number_of)
    heavy_load, common = load_shares(number_of, rows * top, limit, slope, True), load_shares(number_of, rows * top, limit, slope, False)
    places = jnp.arange(number_of)

    def named(tallies, rotation):
        used = int((tallies > 0).sum())
        fixed = max(1, used // 4)
        moved = fixed + (places - fixed + rotation * (used - fixed)) % max(1, number_of - fixed)
        return jnp.zeros((number_of,), jnp.int32).at[sequence[jnp.where(places < fixed, places, moved)]].set(jnp.asarray(tallies, jnp.int32))

    tallies = jnp.where(number % 4 == 0, named(heavy_load, number // 4), named(common, number - number // 4 - 1))
    mixed = jax.random.permutation(jax.random.fold_in(own, 3), number_of)
    source_of, receiver = mixed[0:number_of // 2 * 2:2], mixed[1:number_of // 2 * 2:2]
    room = jnp.minimum(tallies[source_of] - 1, limit - tallies[receiver]) // 2
    room = jnp.where((source_of == sequence[0]) | (receiver == sequence[0]) | (tallies[receiver] == 0), 0, jnp.maximum(room, 0))
    moved = jax.random.randint(jax.random.fold_in(own, 4), (number_of // 2,), 0, 1 << 20) % (room + 1)
    tallies = tallies.at[source_of].add(-moved).at[receiver].add(moved)
    labels = jnp.searchsorted(jnp.cumsum(tallies), jnp.arange(rows * top), side="right").astype(jnp.int32)
    grid = labels.reshape(top, rows).T
    grid = grid[jax.random.permutation(jax.random.fold_in(own, 1), rows)]
    rotation = jax.random.randint(jax.random.fold_in(own, 2), (rows, 1), 0, top)
    return jnp.take_along_axis(grid, (jnp.arange(top)[None, :] + rotation) % top, axis=1)


def load_shares(count, total, reach, slope, full):
    weights = [(1 << 20) // math.isqrt(standing ** slope) + 1 for standing in range(1, count + 1)]
    largest = reach if full else min(reach, max(-(-total // count), total * weights[0] // sum(weights)))
    least = 1 if total - largest >= count - 1 else 0
    given, surplus = [largest] + [least] * (count - 1), total - largest - least * (count - 1)
    while surplus > 0:
        free = [i for i in range(1, count) if given[i] < largest] or [i for i in range(1, count) if given[i] < reach]
        mass, remaining = sum([weights[i] for i in free]), surplus
        for i in free:
            addition = min(reach - given[i], max(1, remaining * weights[i] // mass), surplus)
            given[i] = given[i] + addition
            surplus = surplus - addition
    return np.array(given)


def gaussian(own_key, shape, width, limit, shards=(), kind=jnp.bfloat16):
    factor_of = shard_levels(own_key, shape, shards, -0.22, 0.18) if shards else 1.0
    values = jax.random.normal(own_key, shape, jnp.float32) * width * factor_of
    return jnp.minimum(jnp.maximum(values, -limit), limit).astype(kind)


def setup_inputs(seed: int = 0) -> dict:
    key_list = jax.random.split(jax.random.key(seed), 14)
    hidden_in = gaussian(key_list[0], (TOKENS, D), 1.0, 6.0, ((0, 128),))
    query_latent = draw_query_latent(jax.random.fold_in(key_list[13], 71), 0)
    query_rope = draw_query_rope(jax.random.fold_in(key_list[13], 71), 0)
    cache_latent = draw_cache_latent(jax.random.fold_in(key_list[13], 71), 0)
    cache_rope = draw_cache_rope(jax.random.fold_in(key_list[13], 71), 0)
    lengths = plant(jax.random.randint(key_list[5], (TOKENS,), CTX // 8, CTX + 1), jax.random.fold_in(key_list[5], 1), CTX // 8, CTX).astype(jnp.int32)
    value_up = gaussian(key_list[6], (LAT, HEADS * HEAD_V), (LAT // 16) ** -0.5, 1.0, ((1, 4),))
    out_proj = gaussian(key_list[7], (HEADS * HEAD_V, D), (HEADS * HEAD_V) ** -0.5, 0.09375, ((0, 4),))
    norm_gain = jnp.clip(1.0 + 0.18 * jax.random.normal(key_list[8], (D,), jnp.float32), 0.1, 1.9)
    expert_gate = gaussian(key_list[9], (EXPERTS, D, FF), D ** -0.5, 0.09375, ((0, 128),))
    expert_down = gaussian(key_list[10], (EXPERTS, FF, D), FF ** -0.5, 0.1875, ((0, 128),))
    expert_ids_keys = jax.random.split(jax.random.fold_in(key_list[11], 1), TOKENS // TOK_DEV)
    expert_ids_turns = jax.random.permutation(jax.random.fold_in(key_list[11], 3), TOKENS // TOK_DEV)
    expert_ids = jax.vmap(lambda own, number: shared_out(jax.random.fold_in(key_list[11], 2), own, number, TOK_DEV, EXPERTS, TOPK, CAP, 2))(expert_ids_keys, expert_ids_turns).reshape((TOKENS, TOPK))
    affinity = jnp.clip(jnp.exp(math.log(1.0) - 2.9957323 * jax.random.uniform(key_list[12], (TOKENS, TOPK), jnp.float32) ** shard_levels(key_list[12], (TOKENS, TOPK), ((0, 128),), -0.2, 0.2)), 0.05, 1.0)
    return dict(hidden_in=hidden_in, query_latent=query_latent, query_rope=query_rope, cache_latent=cache_latent, cache_rope=cache_rope, lengths=lengths, value_up=value_up, out_proj=out_proj, norm_gain=norm_gain, expert_gate=expert_gate, expert_down=expert_down, expert_ids=expert_ids, affinity=affinity)


score_scale = 192.0 ** (-0.5)
norm_eps = 1e-06
route_scale = 2.5

def attend(query_latent, query_rope, cache_latent, cache_rope, lengths):
    token_count, head_count, latent_width = query_latent.shape
    rope_width = cache_rope.shape[1]
    context = cache_latent.shape[1]
    latent_wide = cache_latent.astype(jnp.float32)
    query_rot = query_rope.astype(jnp.float32).reshape(token_count, head_count, rope_width)
    scores = jnp.einsum('thl,tpl->thp', query_latent.astype(jnp.float32), latent_wide)
    scores = scores + jnp.einsum('thr,trp->thp', query_rot, cache_rope.astype(jnp.float32))
    scores = scores * score_scale
    position = lax.broadcasted_iota(jnp.int32, (token_count, 1, context), 2)
    scores = jnp.where(position < lengths.astype(jnp.int32)[:, None, None], scores, -jnp.inf)
    row_max = lax.optimization_barrier(jnp.max(scores, axis=2, keepdims=True))
    raised = jnp.exp(scores - row_max)
    attn_weights = (raised / lax.optimization_barrier(jnp.sum(raised, axis=2, keepdims=True))).astype(jnp.bfloat16)
    latent_out = jnp.einsum('thp,tpl->thl', attn_weights.astype(jnp.float32), latent_wide)
    return latent_out.astype(jnp.bfloat16)

def reference(hidden_in, query_latent, query_rope, cache_latent, cache_rope, lengths, value_up, out_proj, norm_gain, expert_gate, expert_down, expert_ids, affinity):
    latent_out = attend(query_latent, query_rope, cache_latent, cache_rope, lengths)
    up_table = value_up.astype(jnp.float32).reshape(LAT, HEADS, HEAD_V)
    per_head = jnp.einsum('thl,lhv->thv', latent_out.astype(jnp.float32), up_table).astype(jnp.bfloat16)
    attn_sum = jnp.dot(per_head.reshape(TOKENS, HEADS * HEAD_V), out_proj, preferred_element_type=jnp.float32)
    hidden = (hidden_in.astype(jnp.float32) + attn_sum).astype(jnp.bfloat16)
    wide_hidden = hidden.astype(jnp.float32)
    inv_norm = lax.rsqrt(lax.optimization_barrier(jnp.mean(wide_hidden * wide_hidden, axis=1, keepdims=True)) + norm_eps)
    normed = (wide_hidden * inv_norm * norm_gain.astype(jnp.float32)).astype(jnp.bfloat16)
    blocks = TOKENS // TOK_DEV
    per_block = TOK_DEV * TOPK
    block_ids = expert_ids.astype(jnp.int32).reshape(blocks, per_block)
    expert_iota = jnp.arange(EXPERTS, dtype=jnp.int32)
    one_hot = (block_ids[:, :, None] == expert_iota[None, None, :]).astype(jnp.int32)
    earlier = jnp.cumsum(one_hot, axis=1) - one_hot
    slot_index = lax.optimization_barrier(jnp.sum(earlier * one_hot, axis=2)).astype(jnp.int32)
    block_number = jnp.arange(blocks, dtype=jnp.int32)[:, None]
    target = (block_ids * (blocks * CAP) + block_number * CAP + slot_index).reshape(-1)
    owner_row = jnp.arange(TOKENS * TOPK, dtype=jnp.int32) // TOPK
    route_weight = route_scale * affinity / lax.optimization_barrier(jnp.sum(affinity, axis=1, keepdims=True))
    source_row = jnp.full((EXPERTS * blocks * CAP,), TOKENS, jnp.int32).at[target].set(owner_row)
    row_weight = jnp.zeros((EXPERTS * blocks * CAP,), jnp.float32).at[target].set(route_weight.reshape(-1))
    padded = jnp.concatenate([normed, jnp.zeros((1, D), jnp.bfloat16)], axis=0)

    def one_expert(total, inputs):
        rows_here, weights_here, gate_here, down_here = inputs
        inner_act = jax.nn.silu(jnp.dot(padded[rows_here], gate_here, preferred_element_type=jnp.float32)).astype(jnp.bfloat16)
        answer = jnp.dot(inner_act, down_here, preferred_element_type=jnp.float32).astype(jnp.bfloat16).astype(jnp.float32)
        return (total.at[rows_here].add(weights_here[:, None] * answer, mode='drop'), None)
    moe_sum = lax.scan(one_expert, jnp.zeros((TOKENS, D), jnp.float32), (source_row.reshape(EXPERTS, -1), row_weight.reshape(EXPERTS, -1), expert_gate, expert_down))[0]
    return (wide_hidden + moe_sum).astype(jnp.bfloat16)
```

```python
import jax
import jax.numpy as jnp
from jax import lax
from jax.experimental import pallas as pl
from jax.experimental.pallas import tpu as pltpu
from jax.sharding import PartitionSpec as P

BF16 = jnp.bfloat16
F32 = jnp.float32
MESH = pl.DeviceIdType.MESH

score_scale = 192.0 ** (-0.5)
norm_eps = 1e-06
route_scale = 2.5

TOK, HEADS, LAT, ROPE, CTX = 16, 64, 512, 64, 128
D, FF, TOPK = 3584, 1024, 8
HLOC = 16
UPW = 1024
GROUP = 4
OUT_CHUNK = 512

DIMS = ((0, 1, 2), (1, 2, 0), (2, 0, 1))
CHUNKS = ((0, 1152, 0), (1152, 1280, 1), (2432, 1152, 2))
STRIDE = (32, 1, 8)


def dot(a, b):
    return jnp.dot(a, b, preferred_element_type=F32)


def dot_nt(a, b):
    return lax.dot_general(a, b, (((1,), (1,)), ((), ())), preferred_element_type=F32)


def iota(shape, dim):
    return lax.broadcasted_iota(jnp.int32, shape, dim)


def coords(row_order, j):
    d1, d2, d3 = DIMS[j]
    part = {d3: row_order // 64, d2: (row_order // 8) % 4, d1: (row_order // 2) % 4}
    return part[0], part[1], part[2], (row_order // 32) % 2, row_order % 2


def slot_index(x, y, z, c, s, j):
    pos = (x, y, z)
    d1, d2, d3 = DIMS[j]
    return pos[d3] * 64 + c * 32 + pos[d2] * 8 + pos[d1] * 2 + s


def layer_kernel(*refs):
    n_chunk = len(CHUNKS)
    it = iter(refs)

    def take(n):
        return [next(it) for _ in range(n)]

    (lens, hid_h, ql_h, qr_h, cl_h, cr_h, vu_h, op_h, ng_h, eg_h, ed_h, ids_h, aff_h) = take(13)
    (out,) = take(1)
    (hid, ql, qr, cl, cr, vu, op, ng, eg, ed, ids, aff) = take(12)
    (ls, lr, ph, ps, pr, hb, hacc) = take(7)
    (mt1, mt2, sel, whi, wlo) = take(5)
    gat = take(n_chunk)
    sx = take(n_chunk)
    ox = take(n_chunk)
    yx = take(n_chunk)
    qx = take(n_chunk)
    px = take(n_chunk)
    ux = take(n_chunk)
    tx = take(n_chunk)
    vx = take(n_chunk)
    (ld, lat_s, lat_r, rs_s, rs_r, m1_s, m1_r, m2_s, m2_r, ex_s, ex_r) = take(11)

    dp = lax.axis_index("dp")
    y = lax.axis_index("tp")
    x, z, c = dp // 8, (dp // 2) % 4, dp % 2
    pos = (x, y, z)
    me = (dp, y)

    def at(d, k, dc=0):
        q = [x, y, z]
        q[d] = (q[d] + k) % 4
        return ((q[0] * 4 + q[2]) * 2 + (c + dc) % 2, q[1])

    peers = [at(d, k, dc) for d in range(3) for k in (1, 2, 3) for dc in (0, 1)] + [at(0, 0, 1)]

    def remote(src, dst, s, r, to):
        return pltpu.make_async_remote_copy(
            src_ref=src, dst_ref=dst, send_sem=s, recv_sem=r, device_id=to, device_id_type=MESH
        )

    barrier = pltpu.get_barrier_semaphore()
    for peer in peers:
        pl.semaphore_signal(barrier, inc=1, device_id=peer, device_id_type=MESH)

    def load(src, dst, sem):
        copy = pltpu.make_async_copy(src, dst, ld.at[sem])
        copy.start()
        return copy

    groups = TOK // GROUP
    att_loads = []
    small = [load(ids_h, ids, 0), load(aff_h, aff, 1)]
    for g in range(groups):
        sl = pl.ds(g * GROUP, GROUP)
        att_loads.append(
            [
                load(ql_h.at[sl], ql.at[sl], 2 + 4 * g),
                load(cl_h.at[sl], cl.at[sl], 3 + 4 * g),
                load(qr_h.at[sl], qr.at[sl], 4 + 4 * g),
                load(cr_h.at[sl], cr.at[sl], 5 + 4 * g),
            ]
        )
    base = 2 + 4 * groups
    vu_load = load(vu_h, vu, base)
    op_load = load(op_h, op, base + 1)
    hid_load = load(hid_h, hid, base + 2)
    ng_load = load(ng_h, ng, base + 3)
    eg_load = load(eg_h.at[0], eg, base + 4)
    ed_load = load(ed_h.at[0], ed, base + 5)

    for copy in small:
        copy.wait()
    ids_f = ids[...].astype(F32)
    affinity = aff[...]
    weight = route_scale * affinity / jnp.sum(affinity, axis=1, keepdims=True)
    w_hi = weight.astype(BF16)
    w_lo = (weight - w_hi.astype(F32)).astype(BF16)
    spread = (iota((TOPK, 128), 1) % TOPK == iota((TOPK, 128), 0)).astype(F32).astype(BF16)
    own_lane = iota((TOK, 128), 1) // TOPK == iota((TOK, 128), 0)

    def to_lanes(v):
        return jnp.sum(jnp.where(own_lane, dot(v, spread), 0.0), axis=0, keepdims=True)

    ids_b = ids_f.astype(BF16)
    id_row = to_lanes(ids_b)
    rep = (iota((128, TOK), 0) // TOPK == iota((128, TOK), 1)).astype(F32).astype(BF16)
    id_col = jnp.sum(
        jnp.where(iota((128, TOPK), 0) % TOPK == iota((128, TOPK), 1), dot(rep, ids_b), 0.0),
        axis=1,
        keepdims=True,
    )
    earlier = (id_col == id_row) & (iota((128, 128), 0) < iota((128, 128), 1))
    slot_row = jnp.sum(jnp.where(earlier, 1.0, 0.0), axis=0, keepdims=True)
    mrow = iota((16, 128), 0)
    meta = jnp.where(
        mrow == 0,
        id_row,
        jnp.where(mrow == 1, slot_row, jnp.where(mrow == 2, to_lanes(w_hi), to_lanes(w_lo))),
    ).astype(BF16)
    for d in range(3):
        mt1[d, pos[d]] = meta

    position = iota((HEADS, CTX), 1)

    def attend(t):
        q, kv = ql[t], cl[t]
        scores = dot_nt(q, kv) + dot(qr[t], cr[t])
        scores = jnp.where(position < lens[t], scores * score_scale, -jnp.inf)
        raised = jnp.exp(scores - jnp.max(scores, axis=1, keepdims=True))
        probs = (raised / jnp.sum(raised, axis=1, keepdims=True)).astype(BF16)
        latent = dot(probs, kv).astype(BF16)
        for g in range(4):
            ls[g, t] = latent[g * HLOC : (g + 1) * HLOC]

    lat_sends = []
    for g in range(groups):
        for copy in att_loads[g]:
            copy.wait()

        def step(i, carry):
            for u in range(2):
                attend(g * GROUP + i * 2 + u)
            return carry

        lax.fori_loop(0, GROUP // 2, step, 0)
        if g == 0:
            pl.semaphore_wait(barrier, len(peers))
        for k in (2, 1, 3):
            to = at(1, k)
            copy = remote(
                ls.at[to[1], pl.ds(g * GROUP, GROUP)],
                lr.at[y, pl.ds(g * GROUP, GROUP)],
                lat_s.at[g, k],
                lat_r.at[g, k],
                to,
            )
            copy.start()
            lat_sends.append(copy)
        if g == 0:
            for d in range(3):
                for k in (1, 2, 3):
                    remote(mt1.at[d, pos[d]], mt1.at[d, pos[d]], m1_s.at[d], m1_r.at[d], at(d, k)).start()

    for j in range(3):
        d1, d2, _ = DIMS[j]
        remote(mt1.at[d1, pl.ds(0, 3)], mt1.at[d1, pl.ds(0, 3)], m1_s.at[d1], m1_r.at[d1], me).wait_recv()
        mt2[j, pos[d2]] = mt1[d1]
    for j in range(3):
        d1, d2, _ = DIMS[j]
        for k in (1, 2, 3):
            remote(mt2.at[j, pos[d2]], mt2.at[j, pos[d2]], m2_s.at[j], m2_r.at[j], at(d2, k)).start()

    vu_load.wait()
    diag = iota((TOK * HLOC, UPW), 0) % HLOC == iota((TOK * HLOC, UPW), 1) // 64
    fold = (iota((TOK, TOK * HLOC), 1) // HLOC == iota((TOK, TOK * HLOC), 0)).astype(F32).astype(BF16)

    def up(latents, src):
        wide = dot(latents.reshape(TOK * HLOC, LAT), vu[...])
        ph[src] = dot(fold, jnp.where(diag, wide, 0.0).astype(BF16)).astype(BF16)

    up(ls[y], y)

    row = iota((256, 128), 0)
    pick_row = iota((256, 256), 0)
    pick_col = iota((256, 256), 1)
    tok_of_lane = (iota((128, 256), 0) // TOPK == iota((128, 256), 1) % TOK).astype(F32).astype(BF16)
    tok_of_lane_t = (iota((256, 128), 1) // TOPK == iota((256, 128), 0) % TOK).astype(F32).astype(BF16)
    for j in range(3):
        _, _, d3 = DIMS[j]
        remote(mt2.at[j, pl.ds(0, 3)], mt2.at[j, pl.ds(0, 3)], m2_s.at[j], m2_r.at[j], me).wait_recv()
        facts = mt2[j].reshape(256, 128)

        def of_source(n):
            hot = pick_col == ((pick_row // 2) % 16) * 16 + n
            return dot(hot.astype(F32).astype(BF16), facts)

        here = sum(pos[d] * STRIDE[d] for d in range(3) if d != d3)
        expert = here + (row // 64) * STRIDE[d3] + ((row // 32) % 2) * 4
        match = (of_source(0) == expert.astype(F32)) & (of_source(1) == (row % 2).astype(F32))
        same = (pick_row // 2) % 16 == pick_col // TOK
        hit = jnp.where(match, 1.0, 0.0).astype(BF16)
        sel[j] = jnp.where(same, dot(hit, tok_of_lane), 0.0).astype(BF16)
        same_t = (pick_col // 2) % 16 == pick_row // TOK
        for n, ref in ((2, whi), (3, wlo)):
            val = jnp.where(match, of_source(n), 0.0).astype(BF16)
            ref[j] = jnp.where(same_t, dot_nt(tok_of_lane_t, val), 0.0).astype(BF16)

    for k in (1, 3, 2):
        for g in range(groups):
            sl = pl.ds(g * GROUP, GROUP)
            remote(ls.at[0, sl], lr.at[0, sl], lat_s.at[g, k], lat_r.at[g, k], me).wait_recv()
        src = (y + 4 - k) % 4
        up(lr[src], src)

    op_load.wait()
    heads_out = ph[...].reshape(4 * TOK, UPW)

    def project(n, carry):
        cols = pl.ds(pl.multiple_of(n * OUT_CHUNK, OUT_CHUNK), OUT_CHUNK)
        part = dot(heads_out, op[:, cols]).astype(BF16)
        ps[:, :, cols] = part.reshape(4, TOK, OUT_CHUNK)
        for k in (2, 1, 3):
            to = at(1, k)
            remote(ps.at[to[1], :, cols], pr.at[y, :, cols], rs_s, rs_r, to).start()
        return carry

    lax.fori_loop(0, D // OUT_CHUNK, project, 0)
    hid_load.wait()
    ng_load.wait()
    pr[y] = ps[y]
    remote(ps.at[pl.ds(0, 3)], pr.at[pl.ds(0, 3)], rs_s, rs_r, me).wait_recv()
    total = hid[...].astype(F32)
    for src in range(4):
        total = total + pr[src].astype(F32)
    hidden = total.astype(BF16)
    hid[...] = hidden
    wide = hidden.astype(F32)
    inv = lax.rsqrt(jnp.mean(wide * wide, axis=1, keepdims=True) + norm_eps)
    normed = (wide * inv * ng[...]).astype(BF16)

    def exchange(ph_no, i, src, dst, to):
        remote(src, dst, ex_s.at[ph_no, i], ex_r.at[ph_no, i], to).start()

    def arrived(ph_no, i, ref, n):
        remote(ref.at[pl.ds(0, n)], ref.at[pl.ds(0, n)], ex_s.at[ph_no, i], ex_r.at[ph_no, i], me).wait_recv()

    line = [(k, dc) for k in (2, 1, 3, 0) for dc in (0, 1) if (k, dc) != (0, 0)]

    def to_line(ph_no, i, d3, src, dst):
        slot = pos[d3] * 2 + c
        for k, dc in line:
            there = ((pos[d3] + k) % 4) * 2 + (c + dc) % 2
            exchange(ph_no, i, src.at[there], dst.at[slot], at(d3, k, dc))
        dst[slot] = src[slot]

    for i, (lo, n, j) in enumerate(CHUNKS):
        d1, d2, d3 = DIMS[j]
        gat[i][pos[d2], pos[d1]] = normed[:, lo : lo + n]
        for k in (2, 1, 3):
            mine = gat[i].at[pos[d2], pos[d1]]
            exchange(0, i, mine, mine, at(d1, k))
    for i, (lo, n, j) in enumerate(CHUNKS):
        d1, d2, d3 = DIMS[j]
        arrived(0, i, gat[i].at[0], 3)
        for k in (2, 1, 3):
            mine = gat[i].at[pos[d2]]
            exchange(1, i, mine, mine, at(d2, k))
    for i, (lo, n, j) in enumerate(CHUNKS):
        d1, d2, d3 = DIMS[j]
        arrived(1, i, gat[i], 3)
        rows = dot(sel[j], gat[i][...].reshape(256, n)).astype(BF16)
        sx[i][...] = rows.reshape(8, 32, n)
        to_line(2, i, d3, sx[i], ox[i])

    def reorder(to_j, from_j):
        want = slot_index(*coords(pick_row, to_j), from_j)
        return (want == pick_col).astype(F32).astype(BF16)

    eg_load.wait()
    for i, (lo, n, j) in enumerate(CHUNKS):
        arrived(2, i, ox[i], 7)
        rows = ox[i][...].reshape(256, n)
        if j != 0:
            rows = dot(reorder(0, j), rows).astype(BF16)
        part = dot(rows, eg[lo : lo + n, :])
        if i == 0:
            hacc[...] = part
        elif i < n_chunk - 1:
            hacc[...] += part
        else:
            v = hacc[...] + part
            hb[...] = (v / (1.0 + jnp.exp(-v))).astype(BF16)
    ed_load.wait()
    for i, (lo, n, j) in enumerate(CHUNKS):
        d1, d2, d3 = DIMS[j]
        rows = dot(hb[...], ed[:, lo : lo + n]).astype(BF16)
        if j != 0:
            rows = dot(reorder(j, 0), rows).astype(BF16)
        yx[i][...] = rows.reshape(8, 32, n)
        to_line(3, i, d3, yx[i], qx[i])

    for i, (lo, n, j) in enumerate(CHUNKS):
        d1, d2, d3 = DIMS[j]
        arrived(3, i, qx[i], 7)
        rows = qx[i][...].reshape(256, n)
        summed = (dot(whi[j], rows) + dot(wlo[j], rows)).astype(BF16)
        px[i][...] = summed.reshape(4, 64, n)
        for k in (2, 1, 3):
            exchange(4, i, px[i].at[(pos[d2] + k) % 4], ux[i].at[pos[d2]], at(d2, k))
        ux[i][pos[d2]] = px[i][pos[d2]]
    for i, (lo, n, j) in enumerate(CHUNKS):
        d1, d2, d3 = DIMS[j]
        arrived(4, i, ux[i], 3)
        acc = ux[i][0].astype(F32)
        for q in range(1, 4):
            acc = acc + ux[i][q].astype(F32)
        tx[i][...] = acc.astype(BF16).reshape(4, TOK, n)
        for k in (2, 1, 3):
            exchange(5, i, tx[i].at[(pos[d1] + k) % 4], vx[i].at[pos[d1]], at(d1, k))
        vx[i][pos[d1]] = tx[i][pos[d1]]
    for i, (lo, n, j) in enumerate(CHUNKS):
        arrived(5, i, vx[i], 3)
        acc = hid[:, lo : lo + n].astype(F32)
        for q in range(4):
            acc = acc + vx[i][q].astype(F32)
        out[:, lo : lo + n] = acc.astype(BF16)

    for copy in lat_sends:
        copy.wait_send()
    remote(ps.at[pl.ds(0, 3)], pr.at[pl.ds(0, 3)], rs_s, rs_r, me).wait_send()
    for d in range(3):
        remote(mt1.at[d, pl.ds(0, 3)], mt1.at[d, pl.ds(0, 3)], m1_s.at[d], m1_r.at[d], me).wait_send()
        remote(mt2.at[d, pl.ds(0, 3)], mt2.at[d, pl.ds(0, 3)], m2_s.at[d], m2_r.at[d], me).wait_send()
    for i in range(n_chunk):
        for ph_no, ref, n in (
            (0, gat[i].at[0], 3),
            (1, gat[i], 3),
            (2, sx[i], 7),
            (3, yx[i], 7),
            (4, px[i], 3),
            (5, tx[i], 3),
        ):
            part = ref.at[pl.ds(0, n)]
            remote(part, part, ex_s.at[ph_no, i], ex_r.at[ph_no, i], me).wait_send()


def per_device(
    hidden_in,
    query_latent,
    query_rope,
    cache_latent,
    cache_rope,
    lengths,
    value_up,
    out_proj,
    norm_gain,
    expert_gate,
    expert_down,
    expert_ids,
    affinity,
):
    n_chunk = len(CHUNKS)
    dma = pltpu.SemaphoreType.DMA
    v = pltpu.VMEM
    scratch = [
        v((TOK, D), BF16),
        v((TOK, HEADS, LAT), BF16),
        v((TOK, HEADS, ROPE), BF16),
        v((TOK, CTX, LAT), BF16),
        v((TOK, ROPE, CTX), BF16),
        v((LAT, UPW), BF16),
        v((UPW, D), BF16),
        v((1, D), F32),
        v((D, FF), BF16),
        v((FF, D), BF16),
        v((TOK, TOPK), jnp.int32),
        v((TOK, TOPK), F32),
        v((4, TOK, HLOC, LAT), BF16),
        v((4, TOK, HLOC, LAT), BF16),
        v((4, TOK, UPW), BF16),
        v((4, TOK, D), BF16),
        v((4, TOK, D), BF16),
        v((256, FF), BF16),
        v((256, FF), F32),
        v((3, 4, 16, 128), BF16),
        v((3, 4, 4, 16, 128), BF16),
        v((3, 256, 256), BF16),
        v((3, 256, 256), BF16),
        v((3, 256, 256), BF16),
    ]
    for shape in ((4, 4, TOK), (8, 32), (8, 32), (8, 32), (8, 32), (4, 64), (4, 64), (4, TOK), (4, TOK)):
        scratch += [v(shape + (n,), BF16) for _, n, _ in CHUNKS]
    scratch += [
        dma((2 + TOK + 6,)),
        dma((TOK // GROUP, 4)),
        dma((TOK // GROUP, 4)),
        dma,
        dma,
        dma((3,)),
        dma((3,)),
        dma((3,)),
        dma((3,)),
        dma((6, n_chunk)),
        dma((6, n_chunk)),
    ]
    anyspace = pl.BlockSpec(memory_space=pl.ANY)
    return pl.pallas_call(
        layer_kernel,
        out_shape=jax.ShapeDtypeStruct((TOK, D), BF16),
        in_specs=[pl.BlockSpec(memory_space=pltpu.SMEM)] + [anyspace] * 12,
        out_specs=pl.BlockSpec(memory_space=pltpu.VMEM),
        scratch_shapes=scratch,
        compiler_params=pltpu.CompilerParams(
            collective_id=0, has_side_effects=True, vmem_limit_bytes=64 * 1024 * 1024 - 65536
        ),
        name="layer",
    )(
        lengths,
        hidden_in,
        query_latent,
        query_rope.reshape(TOK, HEADS, ROPE),
        cache_latent,
        cache_rope,
        value_up,
        out_proj,
        norm_gain.reshape(1, D),
        expert_gate,
        expert_down,
        expert_ids,
        affinity,
    )


def solution(mesh):
    return jax.shard_map(
        per_device,
        mesh=mesh,
        in_specs=(
            P(("dp", "tp"), None),
            P(("dp", "tp"), None, None),
            P(("dp", "tp"), None),
            P(("dp", "tp"), None, None),
            P(("dp", "tp"), None, None),
            P(("dp", "tp")),
            P(None, "tp"),
            P("tp", None),
            P(),
            P(("dp", "tp"), None, None),
            P(("dp", "tp"), None, None),
            P(("dp", "tp"), None),
            P(("dp", "tp"), None),
        ),
        out_specs=P(("dp", "tp"), None),
        check_vma=False,
    )
```

```python
import jax
import jax.numpy as jnp
from jax import lax
from jax.experimental import pallas as pl
from jax.experimental.pallas import tpu as pltpu
from jax.sharding import PartitionSpec as P

BF16 = jnp.bfloat16
F32 = jnp.float32
MESH = pl.DeviceIdType.MESH

score_scale = 192.0 ** (-0.5)
norm_eps = 1e-06
route_scale = 2.5

TOK, HEADS, LAT, ROPE, CTX = 16, 64, 512, 64, 128
D, FF, TOPK = 3584, 1024, 8
HLOC = 16
UPW = 1024
GROUP = 2
UP_TOK = 4
OUT_CHUNK = 512

DIMS = ((0, 1, 2), (1, 2, 0), (2, 0, 1))
CHUNKS = (
    (0, 640, 0), (640, 640, 1), (1280, 640, 2),
    (1920, 512, 0), (2432, 640, 1), (3072, 512, 2),
)
STRIDE = (32, 1, 8)


def dot(a, b):
    return jnp.dot(a, b, preferred_element_type=F32)


def dot_nt(a, b):
    return lax.dot_general(a, b, (((1,), (1,)), ((), ())), preferred_element_type=F32)


def iota(shape, dim):
    return lax.broadcasted_iota(jnp.int32, shape, dim)


def coords(row_order, j):
    d1, d2, d3 = DIMS[j]
    part = {d3: row_order >> 6, d2: (row_order >> 3) & 3, d1: (row_order >> 1) & 3}
    return part[0], part[1], part[2], (row_order >> 5) & 1, row_order & 1


def slot_index(x, y, z, c, s, j):
    pos = (x, y, z)
    d1, d2, d3 = DIMS[j]
    return (pos[d3] << 6) + (c << 5) + (pos[d2] << 3) + (pos[d1] << 1) + s


def hot(mask):
    return jnp.where(mask, 1.0, 0.0).astype(BF16)


def col_iota(n):
    return iota((1, n), 1)


def row_iota(n):
    return iota((n, 1), 0)


def layer_kernel(*refs):
    n_chunk = len(CHUNKS)
    it = iter(refs)

    def take(n):
        return [next(it) for _ in range(n)]

    (lens, hid_h, ql_h, qr_h, cl_h, cr_h, vu_h, op_h, ng_h, eg_h, ed_h, ids_h, aff_h) = take(13)
    (out,) = take(1)
    (hid, ql, qr, pairs, cl, cr, vu, op, ng, eg, ed, ids, aff) = take(13)
    (ls, lr, ps, pr, hb, hacc) = take(6)
    (mt1, mt2, sel, whi, wlo, order_in, order_out) = take(7)
    gat = take(n_chunk)
    sx = take(n_chunk)
    ox = take(n_chunk)
    yx = take(n_chunk)
    qx = take(n_chunk)
    px = take(n_chunk)
    ux = take(n_chunk)
    tx = take(n_chunk)
    vx = take(n_chunk)
    (ld, lat_s, lat_r, rs_s, rs_r, m1_s, m1_r, m2_s, m2_r, ex_s, ex_r) = take(11)

    dp = lax.axis_index("dp")
    y = lax.axis_index("tp")
    x, z, c = dp // 8, (dp // 2) % 4, dp % 2
    pos = (x, y, z)
    me = (dp, y)

    def at(d, k, dc=0):
        q = [x, y, z]
        q[d] = (q[d] + k) % 4
        return ((q[0] * 4 + q[2]) * 2 + (c + dc) % 2, q[1])

    peers = [at(d, k, dc) for d in range(3) for k in (1, 2, 3) for dc in (0, 1)] + [at(0, 0, 1)]

    def remote(src, dst, s, r, to):
        return pltpu.make_async_remote_copy(
            src_ref=src, dst_ref=dst, send_sem=s, recv_sem=r, device_id=to, device_id_type=MESH
        )

    barrier = pltpu.get_barrier_semaphore()
    for peer in peers:
        pl.semaphore_signal(barrier, inc=1, device_id=peer, device_id_type=MESH)

    def load(src, dst, sem):
        copy = pltpu.make_async_copy(src, dst, ld.at[sem])
        copy.start()
        return copy

    groups = TOK // GROUP
    qr_load = load(qr_h, qr, 2)
    small = [load(ids_h, ids, 0), load(aff_h, aff, 1)]

    def att_copies(g):
        sl = pl.ds(g * GROUP, GROUP)
        return [
            pltpu.make_async_copy(src.at[sl], dst.at[sl], ld.at[3 + 3 * g + n])
            for n, (src, dst) in enumerate(((ql_h, ql), (cl_h, cl), (cr_h, cr)))
        ]

    for g in range(groups):
        for copy in att_copies(g):
            copy.start()
    base = 3 + 3 * groups
    vu_load = load(vu_h, vu, base)
    op_load = load(op_h, op, base + 1)
    hid_load = load(hid_h, hid, base + 2)
    ng_load = load(ng_h, ng, base + 3)
    eg_load = load(eg_h.at[0], eg, base + 4)
    ed_load = load(ed_h.at[0], ed, base + 5)

    for copy in small:
        copy.wait()
    ids_f = ids[...].astype(F32)
    affinity = aff[...]
    weight = route_scale * affinity / jnp.sum(affinity, axis=0, keepdims=True)
    w_hi = weight.astype(BF16)
    w_lo = (weight - w_hi.astype(F32)).astype(BF16)
    spread = hot(col_iota(128) & 15 == row_iota(TOK))
    own_lane = col_iota(128) >> 4 == row_iota(TOPK)

    def to_lanes(v):
        return jnp.sum(jnp.where(own_lane, dot(v, spread), 0.0), axis=0, keepdims=True)

    ids_b = ids_f.astype(BF16)
    id_row = to_lanes(ids_b)
    rep = hot(row_iota(128) >> 4 == col_iota(TOPK))
    id_col = jnp.sum(
        jnp.where(row_iota(128) & 15 == col_iota(TOK), dot(rep, ids_b), 0.0), axis=1, keepdims=True
    )
    earlier = (id_col == id_row) & (row_iota(128) < col_iota(128))
    slot_row = jnp.sum(jnp.where(earlier, 1.0, 0.0), axis=0, keepdims=True)
    mrow = iota((16, 128), 0)
    meta = jnp.where(
        mrow == 0,
        id_row,
        jnp.where(mrow == 1, slot_row, jnp.where(mrow == 2, to_lanes(w_hi), to_lanes(w_lo))),
    ).astype(BF16)
    for d in range(3):
        mt1[d, pos[d]] = meta

    position = col_iota(CTX)
    own_half = col_iota(2 * ROPE) >> 6 == row_iota(HEADS) & 1
    pair_row = col_iota(HEADS // 2 * TOK) - ((row_iota(HEADS) >> 1) << 4)
    qr_load.wait()
    for n in range(HEADS // 2):
        pairs[n] = qr[:, n * 2 * ROPE : (n + 1) * 2 * ROPE]

    def attend(t):
        q, kv = ql[t], cl[t]
        pick = hot(pair_row == t)
        rot = dot(pick, pairs[...].reshape(HEADS // 2 * TOK, 2 * ROPE))
        rot = jnp.where(own_half, rot, 0.0).astype(BF16)
        scores = dot_nt(q, kv) + dot(rot, jnp.concatenate([cr[t], cr[t]], axis=0))
        scores = jnp.where(position < lens[t], scores * score_scale, -jnp.inf)
        raised = jnp.exp(scores - jnp.max(scores, axis=1, keepdims=True))
        probs = (raised / jnp.sum(raised, axis=1, keepdims=True)).astype(BF16)
        latent = dot(probs, kv).astype(BF16)
        for g in range(4):
            ls[g, t] = latent[g * HLOC : (g + 1) * HLOC]
        lr[y, t] = ls[y, t]

    def attend_group(g):
        for copy in att_copies(g):
            copy.wait()
        for u in range(GROUP):
            attend(g * GROUP + u)

    def lat_copy(g, k):
        to = at(1, k)
        sl = pl.ds(g * GROUP, GROUP)
        return remote(ls.at[to[1], sl], lr.at[y, sl], lat_s.at[g, k], lat_r.at[g, k], to)

    attend_group(0)
    pl.semaphore_wait(barrier, len(peers))
    for k in (2, 1, 3):
        lat_copy(0, k).start()
    for d in range(3):
        for k in (1, 2, 3):
            remote(mt1.at[d, pos[d]], mt1.at[d, pos[d]], m1_s.at[d], m1_r.at[d], at(d, k)).start()

    def attend_step(g, carry):
        attend_group(g)
        for k in (2, 1, 3):
            lat_copy(g, k).start()
        return carry

    lax.fori_loop(1, groups, attend_step, 0)

    for j in range(3):
        d1, d2, _ = DIMS[j]
        remote(mt1.at[d1, pl.ds(0, 3)], mt1.at[d1, pl.ds(0, 3)], m1_s.at[d1], m1_r.at[d1], me).wait_recv()
        mt2[j, pos[d2]] = mt1[d1]
    for j in range(3):
        d1, d2, _ = DIMS[j]
        for k in (1, 2, 3):
            remote(mt2.at[j, pos[d2]], mt2.at[j, pos[d2]], m2_s.at[j], m2_r.at[j], at(d2, k)).start()

    vu_load.wait()
    up_rows = 4 * UP_TOK * HLOC
    diag = row_iota(up_rows) & (HLOC - 1) == col_iota(UPW) >> 6
    from_row = row_iota(4 * TOK)
    from_col = col_iota(up_rows)
    heads_out = jnp.zeros((4 * TOK, UPW), F32)
    for u in range(TOK // UP_TOK):
        for g in range(u * UP_TOK // GROUP, (u + 1) * UP_TOK // GROUP):
            for k in (1, 3, 2):
                lat_copy(g, k).wait_recv()
        latents = lr[:, pl.ds(u * UP_TOK, UP_TOK)].reshape(up_rows, LAT)
        wide = jnp.where(diag, dot(latents, vu[...]), 0.0).astype(BF16)
        fold = hot(((from_col >> 6) << 4) + u * UP_TOK + ((from_col >> 4) & 3) == from_row)
        heads_out = heads_out + dot(fold, wide)
    heads_out = heads_out.astype(BF16)

    op_load.wait()

    def project(n, carry):
        cols = pl.ds(pl.multiple_of(n * OUT_CHUNK, OUT_CHUNK), OUT_CHUNK)
        part = dot(heads_out, op[:, cols]).astype(BF16)
        ps[:, :, cols] = part.reshape(4, TOK, OUT_CHUNK)
        for k in (2, 1, 3):
            to = at(1, k)
            remote(ps.at[to[1], :, cols], pr.at[y, :, cols], rs_s, rs_r, to).start()
        return carry

    lax.fori_loop(0, D // OUT_CHUNK, project, 0)
    row = row_iota(256)
    col = col_iota(256)
    source = (row >> 1) & 15
    expand = hot(source == col_iota(16))
    gather_fact = hot(((row_iota(64) & 15) << 4) + (row_iota(64) >> 4) == col)

    def facts_of(j):
        d3 = DIMS[j][2]
        packed = dot(gather_fact, mt2[j].reshape(256, 128)).astype(BF16)
        here = sum(pos[d] * STRIDE[d] for d in range(3) if d != d3)
        expert = here + (row >> 6) * STRIDE[d3] + ((row >> 5) & 1) * 4
        ident, slot = dot(expand, packed[0:16]), dot(expand, packed[16:32])
        match = (ident == expert.astype(F32)) & (slot == (row & 1).astype(F32))
        return packed, match

    def build_select(j):
        tok_of_lane = hot(row_iota(128) & 15 == col & 15)
        match = facts_of(j)[1]
        sel[j] = jnp.where(source == col >> 4, dot(hot(match), tok_of_lane), 0.0).astype(BF16)

    def build_weights(j):
        lane_token = hot(col_iota(128) & 15 == row & 15)
        packed, match = facts_of(j)
        for n, ref in ((2, whi), (3, wlo)):
            val = jnp.where(match, dot(expand, packed[16 * n : 16 * n + 16]), 0.0).astype(BF16)
            spread_out = dot_nt(lane_token, val)
            ref[j] = jnp.where((col >> 1) & 15 == row >> 4, spread_out, 0.0).astype(BF16)

    def build_order(j):
        order_in[j - 1] = hot(slot_index(*coords(row, 0), j) == col)
        order_out[j - 1] = hot(slot_index(*coords(row, j), 0) == col)

    for j in range(3):
        remote(mt2.at[j, pl.ds(0, 3)], mt2.at[j, pl.ds(0, 3)], m2_s.at[j], m2_r.at[j], me).wait_recv()
    for j in range(3):
        build_select(j)
    for j in (1, 2):
        build_order(j)

    hid_load.wait()
    ng_load.wait()
    pr[y] = ps[y]
    remote(ps.at[pl.ds(0, 3)], pr.at[pl.ds(0, 3)], rs_s, rs_r, me).wait_recv()
    total = hid[...].astype(F32)
    for src in range(4):
        total = total + pr[src].astype(F32)
    hidden = total.astype(BF16)
    hid[...] = hidden
    wide = hidden.astype(F32)
    inv = lax.rsqrt(jnp.mean(wide * wide, axis=1, keepdims=True) + norm_eps)
    normed = (wide * inv * ng[...].reshape(1, D)).astype(BF16)

    def exchange(ph_no, i, src, dst, to):
        remote(src, dst, ex_s.at[ph_no, i], ex_r.at[ph_no, i], to).start()

    def arrived(ph_no, i, ref, n):
        remote(ref.at[pl.ds(0, n)], ref.at[pl.ds(0, n)], ex_s.at[ph_no, i], ex_r.at[ph_no, i], me).wait_recv()

    line = [(k, dc) for k in (2, 1, 3, 0) for dc in (0, 1) if (k, dc) != (0, 0)]

    def to_line(ph_no, i, d3, src, dst):
        slot = pos[d3] * 2 + c
        for k, dc in line:
            there = ((pos[d3] + k) % 4) * 2 + (c + dc) % 2
            exchange(ph_no, i, src.at[there], dst.at[slot], at(d3, k, dc))
        dst[slot] = src[slot]

    for i, (lo, n, j) in enumerate(CHUNKS):
        d1, d2, d3 = DIMS[j]
        gat[i][pos[d2], pos[d1]] = normed[:, lo : lo + n]
        for k in (2, 1, 3):
            mine = gat[i].at[pos[d2], pos[d1]]
            exchange(0, i, mine, mine, at(d1, k))
    for i, (lo, n, j) in enumerate(CHUNKS):
        d1, d2, d3 = DIMS[j]
        arrived(0, i, gat[i].at[0], 3)
        for k in (2, 1, 3):
            mine = gat[i].at[pos[d2]]
            exchange(1, i, mine, mine, at(d2, k))
    for i, (lo, n, j) in enumerate(CHUNKS):
        d1, d2, d3 = DIMS[j]
        arrived(1, i, gat[i], 3)
        rows = dot(sel[j], gat[i][...].reshape(256, n)).astype(BF16)
        sx[i][...] = rows.reshape(8, 32, n)
        to_line(2, i, d3, sx[i], ox[i])

    for j in range(3):
        build_weights(j)

    eg_load.wait()
    for i, (lo, n, j) in enumerate(CHUNKS):
        arrived(2, i, ox[i], 7)
        rows = ox[i][...].reshape(256, n)
        if j != 0:
            rows = dot(order_in[j - 1], rows).astype(BF16)
        part = dot(rows, eg[lo : lo + n, :])
        if i == 0:
            hacc[...] = part
        elif i < n_chunk - 1:
            hacc[...] += part
        else:
            v = hacc[...] + part
            hb[0] = (v / (1.0 + jnp.exp(-v))).astype(BF16)
    ed_load.wait()
    for i, (lo, n, j) in enumerate(CHUNKS):
        if i in (1, 2):
            hb[j] = dot(order_out[j - 1], hb[0]).astype(BF16)
        rows = dot(hb[j], ed[:, lo : lo + n]).astype(BF16)
        yx[i][...] = rows.reshape(8, 32, n)
        to_line(3, i, DIMS[j][2], yx[i], qx[i])

    for i, (lo, n, j) in enumerate(CHUNKS):
        d1, d2, d3 = DIMS[j]
        arrived(3, i, qx[i], 7)
        rows = qx[i][...].reshape(256, n)
        summed = (dot(whi[j], rows) + dot(wlo[j], rows)).astype(BF16)
        px[i][...] = summed.reshape(4, 64, n)
        for k in (2, 1, 3):
            exchange(4, i, px[i].at[(pos[d2] + k) % 4], ux[i].at[pos[d2]], at(d2, k))
        ux[i][pos[d2]] = px[i][pos[d2]]
    for i, (lo, n, j) in enumerate(CHUNKS):
        d1, d2, d3 = DIMS[j]
        arrived(4, i, ux[i], 3)
        acc = ux[i][0].astype(F32)
        for q in range(1, 4):
            acc = acc + ux[i][q].astype(F32)
        tx[i][...] = acc.astype(BF16).reshape(4, TOK, n)
        for k in (2, 1, 3):
            exchange(5, i, tx[i].at[(pos[d1] + k) % 4], vx[i].at[pos[d1]], at(d1, k))
        vx[i][pos[d1]] = tx[i][pos[d1]]
    for i, (lo, n, j) in enumerate(CHUNKS):
        arrived(5, i, vx[i], 3)
        acc = hid[:, lo : lo + n].astype(F32)
        for q in range(4):
            acc = acc + vx[i][q].astype(F32)
        out[:, lo : lo + n] = acc.astype(BF16)

    for g in range(groups):
        for k in (1, 2, 3):
            lat_copy(g, k).wait_send()
    remote(ps.at[pl.ds(0, 3)], pr.at[pl.ds(0, 3)], rs_s, rs_r, me).wait_send()
    for d in range(3):
        remote(mt1.at[d, pl.ds(0, 3)], mt1.at[d, pl.ds(0, 3)], m1_s.at[d], m1_r.at[d], me).wait_send()
        remote(mt2.at[d, pl.ds(0, 3)], mt2.at[d, pl.ds(0, 3)], m2_s.at[d], m2_r.at[d], me).wait_send()
    for i in range(n_chunk):
        for ph_no, ref, n in (
            (0, gat[i].at[0], 3),
            (1, gat[i], 3),
            (2, sx[i], 7),
            (3, yx[i], 7),
            (4, px[i], 3),
            (5, tx[i], 3),
        ):
            part = ref.at[pl.ds(0, n)]
            remote(part, part, ex_s.at[ph_no, i], ex_r.at[ph_no, i], me).wait_send()


def per_device(
    hidden_in,
    query_latent,
    query_rope,
    cache_latent,
    cache_rope,
    lengths,
    value_up,
    out_proj,
    norm_gain,
    expert_gate,
    expert_down,
    expert_ids,
    affinity,
):
    n_chunk = len(CHUNKS)
    dma = pltpu.SemaphoreType.DMA
    v = pltpu.VMEM
    scratch = [
        v((TOK, D), BF16),
        v((TOK, HEADS, LAT), BF16),
        v((TOK, HEADS * ROPE), BF16),
        v((HEADS // 2, TOK, 2 * ROPE), BF16),
        v((TOK, CTX, LAT), BF16),
        v((TOK, ROPE, CTX), BF16),
        v((LAT, UPW), BF16),
        v((UPW, D), BF16),
        v((D,), F32),
        v((D, FF), BF16),
        v((FF, D), BF16),
        v((TOPK, TOK), jnp.int32),
        v((TOPK, TOK), F32),
        v((4, TOK, HLOC, LAT), BF16),
        v((4, TOK, HLOC, LAT), BF16),
        v((4, TOK, D), BF16),
        v((4, TOK, D), BF16),
        v((3, 256, FF), BF16),
        v((256, FF), F32),
        v((3, 4, 16, 128), BF16),
        v((3, 4, 4, 16, 128), BF16),
        v((3, 256, 256), BF16),
        v((3, 256, 256), BF16),
        v((3, 256, 256), BF16),
        v((2, 256, 256), BF16),
        v((2, 256, 256), BF16),
    ]
    for shape in ((4, 4, TOK), (8, 32), (8, 32), (8, 32), (8, 32), (4, 64), (4, 64), (4, TOK), (4, TOK)):
        scratch += [v(shape + (n,), BF16) for _, n, _ in CHUNKS]
    scratch += [
        dma((3 + 3 * (TOK // GROUP) + 6,)),
        dma((TOK // GROUP, 4)),
        dma((TOK // GROUP, 4)),
        dma,
        dma,
        dma((3,)),
        dma((3,)),
        dma((3,)),
        dma((3,)),
        dma((6, n_chunk)),
        dma((6, n_chunk)),
    ]
    anyspace = pl.BlockSpec(memory_space=pl.ANY)
    return pl.pallas_call(
        layer_kernel,
        out_shape=jax.ShapeDtypeStruct((TOK, D), BF16),
        in_specs=[pl.BlockSpec(memory_space=pltpu.SMEM)] + [anyspace] * 12,
        out_specs=pl.BlockSpec(memory_space=pltpu.VMEM),
        scratch_shapes=scratch,
        compiler_params=pltpu.CompilerParams(
            collective_id=0, has_side_effects=True, vmem_limit_bytes=64 * 1024 * 1024 - 65536
        ),
        name="layer",
    )(
        lengths,
        hidden_in,
        query_latent,
        query_rope,
        cache_latent,
        cache_rope,
        value_up,
        out_proj,
        norm_gain,
        expert_gate,
        expert_down,
        expert_ids.T,
        affinity.T,
    )


def solution(mesh):
    return jax.shard_map(
        per_device,
        mesh=mesh,
        in_specs=(
            P(("dp", "tp"), None),
            P(("dp", "tp"), None, None),
            P(("dp", "tp"), None),
            P(("dp", "tp"), None, None),
            P(("dp", "tp"), None, None),
            P(("dp", "tp")),
            P(None, "tp"),
            P("tp", None),
            P(),
            P(("dp", "tp"), None, None),
            P(("dp", "tp"), None, None),
            P(("dp", "tp"), None),
            P(("dp", "tp"), None),
        ),
        out_specs=P(("dp", "tp"), None),
        check_vma=False,
    )
```

```python
import jax
import jax.numpy as jnp
from jax import lax
from jax.experimental import pallas as pl
from jax.experimental.pallas import tpu as pltpu
from jax.sharding import PartitionSpec as P

BF16 = jnp.bfloat16
F32 = jnp.float32
MESH = pl.DeviceIdType.MESH

score_scale = 192.0 ** (-0.5)
norm_eps = 1e-06
route_scale = 2.5

TOK, HEADS, LAT, ROPE, CTX = 16, 64, 512, 64, 128
D, FF, TOPK = 3584, 1024, 8
HLOC = 16
UPW = 1024
GROUP = 2
UP_TOK = 4

DIMS = ((0, 1, 2), (1, 2, 0), (2, 0, 1))
CHUNKS = ((0, 512, 2), (512, 512, 0), (1024, 512, 1), (1536, 384, 2), (1920, 384, 0), (2304, 384, 1), (2688, 256, 2), (2944, 384, 0), (3328, 256, 1))
WIDTHS = tuple(n for _, n, _ in CHUNKS[:-1]) + (CHUNKS[-1][1] + 128,)
BACK = ((0, 512, 2), (512, 512, 0), (1024, 512, 1), (1536, 384, 2), (1920, 384, 0), (2304, 384, 1), (2688, 256, 2), (2944, 384, 0), (3328, 256, 1))
STRIDE = (32, 1, 8)


def dot(a, b):
    return jnp.dot(a, b, preferred_element_type=F32)


def dot_nt(a, b):
    return lax.dot_general(a, b, (((1,), (1,)), ((), ())), preferred_element_type=F32)


def iota(shape, dim):
    return lax.broadcasted_iota(jnp.int32, shape, dim)


def coords(row_order, j):
    d1, d2, d3 = DIMS[j]
    part = {d3: row_order >> 6, d2: (row_order >> 3) & 3, d1: (row_order >> 1) & 3}
    return part[0], part[1], part[2], (row_order >> 5) & 1, row_order & 1


def slot_index(x, y, z, c, s, j):
    pos = (x, y, z)
    d1, d2, d3 = DIMS[j]
    return (pos[d3] << 6) + (c << 5) + (pos[d2] << 3) + (pos[d1] << 1) + s


def hot(mask):
    return jnp.where(mask, 1.0, 0.0).astype(BF16)


def col_iota(n):
    return iota((1, n), 1)


def row_iota(n):
    return iota((n, 1), 0)


def layer_kernel(*refs):
    n_chunk = len(CHUNKS)
    n_back = len(BACK)
    it = iter(refs)

    def take(n):
        return [next(it) for _ in range(n)]

    (lens, hid_h, ql_h, qr_h, cl_h, cr_h, vu_h, op_h, ng_h, eg_h, ed_h, ids_h, aff_h) = take(13)
    (out,) = take(1)
    (hid, ql, qr, pairs, cl, cr, vu, op, ng, eg, ed, ids, aff) = take(13)
    (ls, lr, ps, pr, hb, hacc) = take(6)
    (mt1, mt2, sel, whi, wlo, order_in, order_out) = take(7)
    gat = take(n_chunk)
    sx = take(n_chunk)
    ox = take(n_chunk)
    yx = take(n_back)
    qx = take(n_back)
    px = take(n_back)
    ux = take(n_back)
    tx = take(n_back)
    vx = take(n_back)
    (ld, lat_s, lat_r, rs_s, rs_r, m1_s, m1_r, m2_s, m2_r, ex_s, ex_r) = take(11)

    dp = lax.axis_index("dp")
    y = lax.axis_index("tp")
    x, z, c = dp // 8, (dp // 2) % 4, dp % 2
    pos = (x, y, z)
    me = (dp, y)

    def at(d, k, dc=0):
        q = [x, y, z]
        q[d] = (q[d] + k) % 4
        return ((q[0] * 4 + q[2]) * 2 + (c + dc) % 2, q[1])

    peers = [at(d, k, dc) for d in range(3) for k in (1, 2, 3) for dc in (0, 1)] + [at(0, 0, 1)]

    def remote(src, dst, s, r, to):
        return pltpu.make_async_remote_copy(
            src_ref=src, dst_ref=dst, send_sem=s, recv_sem=r, device_id=to, device_id_type=MESH
        )

    barrier = pltpu.get_barrier_semaphore()
    for peer in peers:
        pl.semaphore_signal(barrier, inc=1, device_id=peer, device_id_type=MESH)

    def load(src, dst, sem):
        copy = pltpu.make_async_copy(src, dst, ld.at[sem])
        copy.start()
        return copy

    groups = TOK // GROUP
    qr_load = load(qr_h, qr, 2)
    small = [load(ids_h, ids, 0), load(aff_h, aff, 1)]

    def att_copies(g):
        sl = pl.ds(g * GROUP, GROUP)
        return [
            pltpu.make_async_copy(src.at[sl], dst.at[sl], ld.at[3 + 3 * g + n])
            for n, (src, dst) in enumerate(((ql_h, ql), (cl_h, cl), (cr_h, cr)))
        ]

    for g in range(groups):
        for copy in att_copies(g):
            copy.start()
    base = 3 + 3 * groups
    vu_load = load(vu_h, vu, base)
    op_load = load(op_h, op, base + 1)
    hid_load = load(hid_h, hid, base + 2)
    ng_load = load(ng_h, ng, base + 3)
    eg_load = load(eg_h.at[0], eg, base + 4)
    ed_load = load(ed_h.at[0], ed, base + 5)

    position = col_iota(CTX)
    own_half = col_iota(2 * ROPE) >> 6 == row_iota(HEADS) & 1
    pair_row = col_iota(HEADS // 2 * TOK) - ((row_iota(HEADS) >> 1) << 4)
    qr_load.wait()
    for n in range(HEADS // 2):
        pairs[n] = qr[:, n * 2 * ROPE : (n + 1) * 2 * ROPE]

    def attend(t):
        q, kv = ql[t], cl[t]
        pick = hot(pair_row == t)
        rot = dot(pick, pairs[...].reshape(HEADS // 2 * TOK, 2 * ROPE))
        rot = jnp.where(own_half, rot, 0.0).astype(BF16)
        scores = dot_nt(q, kv) + dot(rot, jnp.concatenate([cr[t], cr[t]], axis=0))
        scores = jnp.where(position < lens[t], scores * score_scale, -jnp.inf)
        raised = jnp.exp(scores - jnp.max(scores, axis=1, keepdims=True))
        probs = (raised / jnp.sum(raised, axis=1, keepdims=True)).astype(BF16)
        latent = dot(probs, kv).astype(BF16)
        for g in range(4):
            ls[g, t] = latent[g * HLOC : (g + 1) * HLOC]
        lr[y, t] = ls[y, t]

    def attend_group(g):
        for copy in att_copies(g):
            copy.wait()
        for u in range(GROUP):
            attend(g * GROUP + u)

    def lat_copy(g, k):
        to = at(1, k)
        sl = pl.ds(g * GROUP, GROUP)
        return remote(ls.at[to[1], sl], lr.at[y, sl], lat_s.at[g, k], lat_r.at[g, k], to)

    attend_group(0)
    pl.semaphore_wait(barrier, len(peers))
    for k in (2, 1, 3):
        lat_copy(0, k).start()
    for copy in small:
        copy.wait()
    ids_f = ids[...].astype(F32)
    affinity = aff[...]
    weight = route_scale * affinity / jnp.sum(affinity, axis=0, keepdims=True)
    w_hi = weight.astype(BF16)
    w_lo = (weight - w_hi.astype(F32)).astype(BF16)
    spread = hot(col_iota(128) & 15 == row_iota(TOK))
    own_lane = col_iota(128) >> 4 == row_iota(TOPK)

    def to_lanes(v):
        return jnp.sum(jnp.where(own_lane, dot(v, spread), 0.0), axis=0, keepdims=True)

    ids_b = ids_f.astype(BF16)
    id_row = to_lanes(ids_b)
    rep = hot(row_iota(128) >> 4 == col_iota(TOPK))
    id_col = jnp.sum(
        jnp.where(row_iota(128) & 15 == col_iota(TOK), dot(rep, ids_b), 0.0), axis=1, keepdims=True
    )
    earlier = (id_col == id_row) & (row_iota(128) < col_iota(128))
    slot_row = jnp.sum(jnp.where(earlier, 1.0, 0.0), axis=0, keepdims=True)
    mrow = iota((16, 128), 0)
    meta = jnp.where(
        mrow == 0,
        id_row,
        jnp.where(mrow == 1, slot_row, jnp.where(mrow == 2, to_lanes(w_hi), to_lanes(w_lo))),
    ).astype(BF16)
    for d in range(3):
        mt1[d, pos[d]] = meta

    for d in range(3):
        for k in (1, 2, 3):
            remote(mt1.at[d, pos[d]], mt1.at[d, pos[d]], m1_s.at[d], m1_r.at[d], at(d, k)).start()

    def attend_step(g, carry):
        attend_group(g)
        for k in (2, 1, 3):
            lat_copy(g, k).start()
        return carry

    lax.fori_loop(1, groups, attend_step, 0)

    for j in range(3):
        d1, d2, _ = DIMS[j]
        remote(mt1.at[d1, pl.ds(0, 3)], mt1.at[d1, pl.ds(0, 3)], m1_s.at[d1], m1_r.at[d1], me).wait_recv()
        mt2[j, pos[d2]] = mt1[d1]
    for j in range(3):
        d1, d2, _ = DIMS[j]
        for k in (1, 2, 3):
            remote(mt2.at[j, pos[d2]], mt2.at[j, pos[d2]], m2_s.at[j], m2_r.at[j], at(d2, k)).start()

    vu_load.wait()
    up_rows = 4 * UP_TOK * HLOC
    diag = row_iota(up_rows) & (HLOC - 1) == col_iota(UPW) >> 6
    from_row = row_iota(4 * TOK)
    from_col = col_iota(up_rows)
    heads_out = jnp.zeros((4 * TOK, UPW), F32)
    for u in range(TOK // UP_TOK):
        for g in range(u * UP_TOK // GROUP, (u + 1) * UP_TOK // GROUP):
            for k in (1, 3, 2):
                lat_copy(g, k).wait_recv()
        latents = lr[:, pl.ds(u * UP_TOK, UP_TOK)].reshape(up_rows, LAT)
        wide = jnp.where(diag, dot(latents, vu[...]), 0.0).astype(BF16)
        fold = hot(((from_col >> 6) << 4) + u * UP_TOK + ((from_col >> 4) & 3) == from_row)
        heads_out = heads_out + dot(fold, wide)
    heads_out = heads_out.astype(BF16)

    op_load.wait()
    for i, (lo, n, j) in enumerate(CHUNKS):
        part = dot(heads_out, op[:, lo : lo + n]).astype(BF16)
        ps[:, :, lo : lo + n] = part.reshape(4, TOK, n)
        for k in (2, 1, 3):
            to = at(1, k)
            cols = pl.ds(lo, n)
            remote(ps.at[to[1], :, cols], pr.at[y, :, cols], rs_s.at[i], rs_r.at[i], to).start()

    def exchange(ph_no, i, src, dst, to):
        remote(src, dst, ex_s.at[ph_no, i], ex_r.at[ph_no, i], to).start()

    def arrived(ph_no, i, ref, n):
        remote(ref.at[pl.ds(0, n)], ref.at[pl.ds(0, n)], ex_s.at[ph_no, i], ex_r.at[ph_no, i], me).wait_recv()

    line = [(k, dc) for k in (2, 1, 3, 0) for dc in (0, 1) if (k, dc) != (0, 0)]

    def to_line(ph_no, i, d3, src, dst):
        slot = pos[d3] * 2 + c
        for k, dc in line:
            there = ((pos[d3] + k) % 4) * 2 + (c + dc) % 2
            exchange(ph_no, i, src.at[there], dst.at[slot], at(d3, k, dc))
        dst[slot] = src[slot]

    hid_load.wait()
    ng_load.wait()
    gain = ng[...].reshape(1, D)
    pr[y] = ps[y]
    squares = jnp.zeros((TOK, 1), F32)
    for i, (lo, n, j) in enumerate(CHUNKS):
        d1, d2, d3 = DIMS[j]
        cols = pl.ds(lo, n)
        got = pr.at[pl.ds(0, 3), :, cols]
        remote(got, got, rs_s.at[i], rs_r.at[i], me).wait_recv()
        total = hid[:, lo : lo + n].astype(F32)
        for src in range(4):
            total = total + pr[src, :, lo : lo + n].astype(F32)
        hidden = total.astype(BF16)
        hid[:, lo : lo + n] = hidden
        wide = hidden.astype(F32)
        squares = squares + jnp.sum(wide * wide, axis=1, keepdims=True)
        scaled = (wide * gain[:, lo : lo + n]).astype(BF16)
        if i == n_chunk - 1:
            inv = lax.rsqrt(squares / D + norm_eps)
            inv_hi = inv.astype(BF16).astype(F32)
            lane = col_iota(128)
            extra = jnp.where(lane == 0, inv_hi, jnp.where(lane == 1, inv - inv_hi, 0.0))
            scaled = jnp.concatenate([scaled, extra.astype(BF16)], axis=1)
        gat[i][pos[d2], pos[d1]] = scaled
        for k in (2, 1, 3):
            mine = gat[i].at[pos[d2], pos[d1]]
            exchange(0, i, mine, mine, at(d1, k))

    row = row_iota(256)
    col = col_iota(256)
    source = (row >> 1) & 15
    expand = hot(source == col_iota(16))
    gather_fact = hot(((row_iota(64) & 15) << 4) + (row_iota(64) >> 4) == col)

    def facts_of(j):
        d3 = DIMS[j][2]
        packed = dot(gather_fact, mt2[j].reshape(256, 128)).astype(BF16)
        here = sum(pos[d] * STRIDE[d] for d in range(3) if d != d3)
        expert = here + (row >> 6) * STRIDE[d3] + ((row >> 5) & 1) * 4
        ident, slot = dot(expand, packed[0:16]), dot(expand, packed[16:32])
        match = (ident == expert.astype(F32)) & (slot == (row & 1).astype(F32))
        return packed, match

    def build_select(j):
        tok_of_lane = hot(row_iota(128) & 15 == col & 15)
        match = facts_of(j)[1]
        sel[j] = jnp.where(source == col >> 4, dot(hot(match), tok_of_lane), 0.0).astype(BF16)

    def build_weights(j):
        lane_token = hot(col_iota(128) & 15 == row & 15)
        packed, match = facts_of(j)
        for n, ref in ((2, whi), (3, wlo)):
            val = jnp.where(match, dot(expand, packed[16 * n : 16 * n + 16]), 0.0).astype(BF16)
            spread_out = dot_nt(lane_token, val)
            ref[j] = jnp.where((col >> 1) & 15 == row >> 4, spread_out, 0.0).astype(BF16)

    def build_order(j):
        order_in[j - 1] = hot(slot_index(*coords(row, 0), j) == col)
        order_out[j - 1] = hot(slot_index(*coords(row, j), 0) == col)

    for j in range(3):
        remote(mt2.at[j, pl.ds(0, 3)], mt2.at[j, pl.ds(0, 3)], m2_s.at[j], m2_r.at[j], me).wait_recv()
    for j in range(3):
        build_select(j)
    for j in (1, 2):
        build_order(j)

    for i, (lo, n, j) in enumerate(CHUNKS):
        d1, d2, d3 = DIMS[j]
        arrived(0, i, gat[i].at[0], 3)
        for k in (2, 1, 3):
            mine = gat[i].at[pos[d2]]
            exchange(1, i, mine, mine, at(d2, k))
    for i, (lo, n, j) in enumerate(CHUNKS):
        d1, d2, d3 = DIMS[j]
        arrived(1, i, gat[i], 3)
        rows = dot(sel[j], gat[i][...].reshape(256, WIDTHS[i])).astype(BF16)
        sx[i][...] = rows.reshape(8, 32, WIDTHS[i])
        to_line(2, i, d3, sx[i], ox[i])

    for j in range(3):
        build_weights(j)

    eg_load.wait()
    for i, (lo, n, j) in enumerate(CHUNKS):
        arrived(2, i, ox[i], 7)
        rows = ox[i][...].reshape(256, WIDTHS[i])
        if j != 0:
            rows = dot(order_in[j - 1], rows).astype(BF16)
        part = dot(rows[:, :n], eg[lo : lo + n, :])
        if i == 0:
            hacc[...] = part
        elif i < n_chunk - 1:
            hacc[...] += part
        else:
            inv = rows[:, n : n + 1].astype(F32) + rows[:, n + 1 : n + 2].astype(F32)
            v = (hacc[...] + part) * inv
            hb[0] = (v / (1.0 + jnp.exp(-v))).astype(BF16)
    ed_load.wait()
    for i, (lo, n, j) in enumerate(BACK):
        if i < 3 and j != 0:
            hb[j] = dot(order_out[j - 1], hb[0]).astype(BF16)
        rows = dot(hb[j], ed[:, lo : lo + n]).astype(BF16)
        yx[i][...] = rows.reshape(8, 32, n)
        to_line(3, i, DIMS[j][2], yx[i], qx[i])

    for i, (lo, n, j) in enumerate(BACK):
        d1, d2, d3 = DIMS[j]
        arrived(3, i, qx[i], 7)
        rows = qx[i][...].reshape(256, n)
        summed = (dot(whi[j], rows) + dot(wlo[j], rows)).astype(BF16)
        px[i][...] = summed.reshape(4, 64, n)
        for k in (2, 1, 3):
            exchange(4, i, px[i].at[(pos[d2] + k) % 4], ux[i].at[pos[d2]], at(d2, k))
        ux[i][pos[d2]] = px[i][pos[d2]]
    for i, (lo, n, j) in enumerate(BACK):
        d1, d2, d3 = DIMS[j]
        arrived(4, i, ux[i], 3)
        acc = ux[i][0].astype(F32)
        for q in range(1, 4):
            acc = acc + ux[i][q].astype(F32)
        tx[i][...] = acc.astype(BF16).reshape(4, TOK, n)
        for k in (2, 1, 3):
            exchange(5, i, tx[i].at[(pos[d1] + k) % 4], vx[i].at[pos[d1]], at(d1, k))
        vx[i][pos[d1]] = tx[i][pos[d1]]
    for i, (lo, n, j) in enumerate(BACK):
        arrived(5, i, vx[i], 3)
        acc = hid[:, lo : lo + n].astype(F32)
        for q in range(4):
            acc = acc + vx[i][q].astype(F32)
        out[:, lo : lo + n] = acc.astype(BF16)

    for g in range(groups):
        for k in (1, 2, 3):
            lat_copy(g, k).wait_send()
    for i, (lo, n, j) in enumerate(CHUNKS):
        left = ps.at[pl.ds(0, 3), :, pl.ds(lo, n)]
        remote(left, left, rs_s.at[i], rs_r.at[i], me).wait_send()
    for d in range(3):
        remote(mt1.at[d, pl.ds(0, 3)], mt1.at[d, pl.ds(0, 3)], m1_s.at[d], m1_r.at[d], me).wait_send()
        remote(mt2.at[d, pl.ds(0, 3)], mt2.at[d, pl.ds(0, 3)], m2_s.at[d], m2_r.at[d], me).wait_send()
    def left(ph_no, i, ref, n):
        part = ref.at[pl.ds(0, n)]
        remote(part, part, ex_s.at[ph_no, i], ex_r.at[ph_no, i], me).wait_send()

    for i in range(n_chunk):
        left(0, i, gat[i].at[0], 3)
        left(1, i, gat[i], 3)
        left(2, i, sx[i], 7)
    for i in range(n_back):
        left(3, i, yx[i], 7)
        left(4, i, px[i], 3)
        left(5, i, tx[i], 3)


def per_device(
    hidden_in,
    query_latent,
    query_rope,
    cache_latent,
    cache_rope,
    lengths,
    value_up,
    out_proj,
    norm_gain,
    expert_gate,
    expert_down,
    expert_ids,
    affinity,
):
    n_chunk = len(CHUNKS)
    n_back = len(BACK)
    dma = pltpu.SemaphoreType.DMA
    v = pltpu.VMEM
    scratch = [
        v((TOK, D), BF16),
        v((TOK, HEADS, LAT), BF16),
        v((TOK, HEADS * ROPE), BF16),
        v((HEADS // 2, TOK, 2 * ROPE), BF16),
        v((TOK, CTX, LAT), BF16),
        v((TOK, ROPE, CTX), BF16),
        v((LAT, UPW), BF16),
        v((UPW, D), BF16),
        v((D,), F32),
        v((D, FF), BF16),
        v((FF, D), BF16),
        v((TOPK, TOK), jnp.int32),
        v((TOPK, TOK), F32),
        v((4, TOK, HLOC, LAT), BF16),
        v((4, TOK, HLOC, LAT), BF16),
        v((4, TOK, D), BF16),
        v((4, TOK, D), BF16),
        v((3, 256, FF), BF16),
        v((256, FF), F32),
        v((3, 4, 16, 128), BF16),
        v((3, 4, 4, 16, 128), BF16),
        v((3, 256, 256), BF16),
        v((3, 256, 256), BF16),
        v((3, 256, 256), BF16),
        v((2, 256, 256), BF16),
        v((2, 256, 256), BF16),
    ]
    for shape in ((4, 4, TOK), (8, 32), (8, 32)):
        scratch += [v(shape + (n,), BF16) for n in WIDTHS]
    for shape in ((8, 32), (8, 32), (4, 64), (4, 64), (4, TOK), (4, TOK)):
        scratch += [v(shape + (n,), BF16) for _, n, _ in BACK]
    scratch += [
        dma((3 + 3 * (TOK // GROUP) + 6,)),
        dma((TOK // GROUP, 4)),
        dma((TOK // GROUP, 4)),
        dma((n_chunk,)),
        dma((n_chunk,)),
        dma((3,)),
        dma((3,)),
        dma((3,)),
        dma((3,)),
        dma((6, max(n_chunk, n_back))),
        dma((6, max(n_chunk, n_back))),
    ]
    anyspace = pl.BlockSpec(memory_space=pl.ANY)
    return pl.pallas_call(
        layer_kernel,
        out_shape=jax.ShapeDtypeStruct((TOK, D), BF16),
        in_specs=[pl.BlockSpec(memory_space=pltpu.SMEM)] + [anyspace] * 12,
        out_specs=pl.BlockSpec(memory_space=pltpu.VMEM),
        scratch_shapes=scratch,
        compiler_params=pltpu.CompilerParams(
            collective_id=0, has_side_effects=True, vmem_limit_bytes=64 * 1024 * 1024 - 65536
        ),
        name="layer",
    )(
        lengths,
        hidden_in,
        query_latent,
        query_rope,
        cache_latent,
        cache_rope,
        value_up,
        out_proj,
        norm_gain,
        expert_gate,
        expert_down,
        expert_ids.T,
        affinity.T,
    )


def solution(mesh):
    return jax.shard_map(
        per_device,
        mesh=mesh,
        in_specs=(
            P(("dp", "tp"), None),
            P(("dp", "tp"), None, None),
            P(("dp", "tp"), None),
            P(("dp", "tp"), None, None),
            P(("dp", "tp"), None, None),
            P(("dp", "tp")),
            P(None, "tp"),
            P("tp", None),
            P(),
            P(("dp", "tp"), None, None),
            P(("dp", "tp"), None, None),
            P(("dp", "tp"), None),
            P(("dp", "tp"), None),
        ),
        out_specs=P(("dp", "tp"), None),
        check_vma=False,
    )
```

```python
import jax
import jax.numpy as jnp
from jax import lax
from jax.experimental import pallas as pl
from jax.experimental.pallas import tpu as pltpu
from jax.sharding import PartitionSpec as P

BF16 = jnp.bfloat16
F32 = jnp.float32
MESH = pl.DeviceIdType.MESH

score_scale = 192.0 ** (-0.5)
norm_eps = 1e-06
route_scale = 2.5

TOK, HEADS, LAT, ROPE, CTX = 16, 64, 512, 64, 128
D, FF, TOPK = 3584, 1024, 8
HLOC = 16
UPW = 1024
GROUP = 2
UP_TOK = 4

DIMS = ((0, 1, 2), (1, 2, 0), (2, 0, 1))
CHUNKS = ((0, 512, 2), (512, 512, 0), (1024, 512, 1), (1536, 384, 2), (1920, 384, 0), (2304, 384, 1), (2688, 256, 2), (2944, 384, 0), (3328, 256, 1))
WIDTHS = tuple(n for _, n, _ in CHUNKS[:-1]) + (CHUNKS[-1][1] + 128,)
BACK = ((0, 256, 2), (256, 256, 0), (512, 256, 1), (768, 512, 2), (1280, 512, 0), (1792, 512, 1), (2304, 384, 2), (2688, 512, 0), (3200, 384, 1))
STRIDE = (32, 1, 8)


def dot(a, b):
    return jnp.dot(a, b, preferred_element_type=F32)


def dot_nt(a, b):
    return lax.dot_general(a, b, (((1,), (1,)), ((), ())), preferred_element_type=F32)


def iota(shape, dim):
    return lax.broadcasted_iota(jnp.int32, shape, dim)


def coords(row_order, j):
    d1, d2, d3 = DIMS[j]
    part = {d3: row_order >> 6, d2: (row_order >> 3) & 3, d1: (row_order >> 1) & 3}
    return part[0], part[1], part[2], (row_order >> 5) & 1, row_order & 1


def slot_index(x, y, z, c, s, j):
    pos = (x, y, z)
    d1, d2, d3 = DIMS[j]
    return (pos[d3] << 6) + (c << 5) + (pos[d2] << 3) + (pos[d1] << 1) + s


def hot(mask):
    return jnp.where(mask, 1.0, 0.0).astype(BF16)


def col_iota(n):
    return iota((1, n), 1)


def row_iota(n):
    return iota((n, 1), 0)


def layer_kernel(*refs):
    n_chunk = len(CHUNKS)
    n_back = len(BACK)
    it = iter(refs)

    def take(n):
        return [next(it) for _ in range(n)]

    (lens, hid_h, ql_h, qr_h, cl_h, cr_h, vu_h, op_h, ng_h, eg_h, ed_h, ids_h, aff_h) = take(13)
    (out,) = take(1)
    (hid, ql, qr, pairs, cl, cr, vu, op, ng, eg, ed, ids, aff) = take(13)
    (ls, lr, ps, pr, hb, hacc) = take(6)
    (mt1, mt2, sel, whi, wlo, order_in, order_out) = take(7)
    gat = take(n_chunk)
    sx = take(n_chunk)
    ox = take(n_chunk)
    yx = take(n_back)
    qx = take(n_back)
    px = take(n_back)
    ux = take(n_back)
    tx = take(n_back)
    vx = take(n_back)
    (ld, lat_s, lat_r, rs_s, rs_r, m1_s, m1_r, m2_s, m2_r, ex_s, ex_r) = take(11)

    dp = lax.axis_index("dp")
    y = lax.axis_index("tp")
    x, z, c = dp // 8, (dp // 2) % 4, dp % 2
    pos = (x, y, z)
    me = (dp, y)

    def at(d, k, dc=0):
        q = [x, y, z]
        q[d] = (q[d] + k) % 4
        return ((q[0] * 4 + q[2]) * 2 + (c + dc) % 2, q[1])

    peers = [at(d, k, dc) for d in range(3) for k in (1, 2, 3) for dc in (0, 1)] + [at(0, 0, 1)]

    def remote(src, dst, s, r, to):
        return pltpu.make_async_remote_copy(
            src_ref=src, dst_ref=dst, send_sem=s, recv_sem=r, device_id=to, device_id_type=MESH
        )

    barrier = pltpu.get_barrier_semaphore()
    for peer in peers:
        pl.semaphore_signal(barrier, inc=1, device_id=peer, device_id_type=MESH)

    def load(src, dst, sem):
        copy = pltpu.make_async_copy(src, dst, ld.at[sem])
        copy.start()
        return copy

    groups = TOK // GROUP
    qr_load = load(qr_h, qr, 2)
    small = [load(ids_h, ids, 0), load(aff_h, aff, 1)]

    def att_copies(g):
        sl = pl.ds(g * GROUP, GROUP)
        return [
            pltpu.make_async_copy(src.at[sl], dst.at[sl], ld.at[3 + 3 * g + n])
            for n, (src, dst) in enumerate(((ql_h, ql), (cl_h, cl), (cr_h, cr)))
        ]

    for g in range(groups):
        for copy in att_copies(g):
            copy.start()
    base = 3 + 3 * groups
    vu_load = load(vu_h, vu, base)
    op_load = load(op_h, op, base + 1)
    hid_load = load(hid_h, hid, base + 2)
    ng_load = load(ng_h, ng, base + 3)
    eg_load = load(eg_h.at[0], eg, base + 4)
    ed_load = load(ed_h.at[0], ed, base + 5)

    position = col_iota(CTX)
    own_half = col_iota(2 * ROPE) >> 6 == row_iota(HEADS) & 1
    pair_row = col_iota(HEADS // 2 * TOK) - ((row_iota(HEADS) >> 1) << 4)
    qr_load.wait()
    for n in range(HEADS // 2):
        pairs[n] = qr[:, n * 2 * ROPE : (n + 1) * 2 * ROPE]

    def attend(t):
        q, kv = ql[t], cl[t]
        pick = hot(pair_row == t)
        rot = dot(pick, pairs[...].reshape(HEADS // 2 * TOK, 2 * ROPE))
        rot = jnp.where(own_half, rot, 0.0).astype(BF16)
        scores = dot_nt(q, kv) + dot(rot, jnp.concatenate([cr[t], cr[t]], axis=0))
        scores = jnp.where(position < lens[t], scores * score_scale, -jnp.inf)
        raised = jnp.exp(scores - jnp.max(scores, axis=1, keepdims=True))
        probs = (raised / jnp.sum(raised, axis=1, keepdims=True)).astype(BF16)
        latent = dot(probs, kv).astype(BF16)
        for g in range(4):
            ls[g, t] = latent[g * HLOC : (g + 1) * HLOC]
        lr[y, t] = ls[y, t]

    def attend_group(g):
        for copy in att_copies(g):
            copy.wait()
        for u in range(GROUP):
            attend(g * GROUP + u)

    def lat_copy(g, k):
        to = at(1, k)
        sl = pl.ds(g * GROUP, GROUP)
        return remote(ls.at[to[1], sl], lr.at[y, sl], lat_s.at[g, k], lat_r.at[g, k], to)

    attend_group(0)
    pl.semaphore_wait(barrier, len(peers))
    for k in (2, 1, 3):
        lat_copy(0, k).start()
    for copy in small:
        copy.wait()
    ids_f = ids[...].astype(F32)
    affinity = aff[...]
    weight = route_scale * affinity / jnp.sum(affinity, axis=0, keepdims=True)
    w_hi = weight.astype(BF16)
    w_lo = (weight - w_hi.astype(F32)).astype(BF16)
    spread = hot(col_iota(128) & 15 == row_iota(TOK))
    own_lane = col_iota(128) >> 4 == row_iota(TOPK)

    def to_lanes(v):
        return jnp.sum(jnp.where(own_lane, dot(v, spread), 0.0), axis=0, keepdims=True)

    ids_b = ids_f.astype(BF16)
    id_row = to_lanes(ids_b)
    rep = hot(row_iota(128) >> 4 == col_iota(TOPK))
    id_col = jnp.sum(
        jnp.where(row_iota(128) & 15 == col_iota(TOK), dot(rep, ids_b), 0.0), axis=1, keepdims=True
    )
    earlier = (id_col == id_row) & (row_iota(128) < col_iota(128))
    slot_row = jnp.sum(jnp.where(earlier, 1.0, 0.0), axis=0, keepdims=True)
    mrow = iota((16, 128), 0)
    meta = jnp.where(
        mrow == 0,
        id_row,
        jnp.where(mrow == 1, slot_row, jnp.where(mrow == 2, to_lanes(w_hi), to_lanes(w_lo))),
    ).astype(BF16)
    for d in range(3):
        mt1[d, pos[d]] = meta

    for d in range(3):
        for k in (1, 2, 3):
            remote(mt1.at[d, pos[d]], mt1.at[d, pos[d]], m1_s.at[d], m1_r.at[d], at(d, k)).start()

    def attend_step(g, carry):
        attend_group(g)
        for k in (2, 1, 3):
            lat_copy(g, k).start()
        return carry

    lax.fori_loop(1, groups, attend_step, 0)

    for j in range(3):
        d1, d2, _ = DIMS[j]
        remote(mt1.at[d1, pl.ds(0, 3)], mt1.at[d1, pl.ds(0, 3)], m1_s.at[d1], m1_r.at[d1], me).wait_recv()
        mt2[j, pos[d2]] = mt1[d1]
    for j in range(3):
        d1, d2, _ = DIMS[j]
        for k in (1, 2, 3):
            remote(mt2.at[j, pos[d2]], mt2.at[j, pos[d2]], m2_s.at[j], m2_r.at[j], at(d2, k)).start()

    vu_load.wait()
    up_rows = 4 * UP_TOK * HLOC
    diag = row_iota(up_rows) & (HLOC - 1) == col_iota(UPW) >> 6
    from_row = row_iota(4 * TOK)
    from_col = col_iota(up_rows)
    heads_out = jnp.zeros((4 * TOK, UPW), F32)
    for u in range(TOK // UP_TOK):
        for g in range(u * UP_TOK // GROUP, (u + 1) * UP_TOK // GROUP):
            for k in (1, 3, 2):
                lat_copy(g, k).wait_recv()
        latents = lr[:, pl.ds(u * UP_TOK, UP_TOK)].reshape(up_rows, LAT)
        wide = jnp.where(diag, dot(latents, vu[...]), 0.0).astype(BF16)
        fold = hot(((from_col >> 6) << 4) + u * UP_TOK + ((from_col >> 4) & 3) == from_row)
        heads_out = heads_out + dot(fold, wide)
    heads_out = heads_out.astype(BF16)

    op_load.wait()
    for i, (lo, n, j) in enumerate(CHUNKS):
        part = dot(heads_out, op[:, lo : lo + n]).astype(BF16)
        ps[:, :, lo : lo + n] = part.reshape(4, TOK, n)
        for k in (2, 1, 3):
            to = at(1, k)
            cols = pl.ds(lo, n)
            remote(ps.at[to[1], :, cols], pr.at[y, :, cols], rs_s.at[i], rs_r.at[i], to).start()

    def exchange(ph_no, i, src, dst, to):
        remote(src, dst, ex_s.at[ph_no, i], ex_r.at[ph_no, i], to).start()

    def arrived(ph_no, i, ref, n):
        remote(ref.at[pl.ds(0, n)], ref.at[pl.ds(0, n)], ex_s.at[ph_no, i], ex_r.at[ph_no, i], me).wait_recv()

    line = [(k, dc) for k in (2, 1, 3, 0) for dc in (0, 1) if (k, dc) != (0, 0)]

    def to_line(ph_no, i, d3, src, dst):
        slot = pos[d3] * 2 + c
        for k, dc in line:
            there = ((pos[d3] + k) % 4) * 2 + (c + dc) % 2
            exchange(ph_no, i, src.at[there], dst.at[slot], at(d3, k, dc))
        dst[slot] = src[slot]

    hid_load.wait()
    ng_load.wait()
    gain = ng[...].reshape(1, D)
    pr[y] = ps[y]
    squares = jnp.zeros((TOK, 1), F32)
    for i, (lo, n, j) in enumerate(CHUNKS):
        d1, d2, d3 = DIMS[j]
        cols = pl.ds(lo, n)
        got = pr.at[pl.ds(0, 3), :, cols]
        remote(got, got, rs_s.at[i], rs_r.at[i], me).wait_recv()
        total = hid[:, lo : lo + n].astype(F32)
        for src in range(4):
            total = total + pr[src, :, lo : lo + n].astype(F32)
        hidden = total.astype(BF16)
        hid[:, lo : lo + n] = hidden
        wide = hidden.astype(F32)
        squares = squares + jnp.sum(wide * wide, axis=1, keepdims=True)
        scaled = (wide * gain[:, lo : lo + n]).astype(BF16)
        if i == n_chunk - 1:
            inv = lax.rsqrt(squares / D + norm_eps)
            inv_hi = inv.astype(BF16).astype(F32)
            lane = col_iota(128)
            extra = jnp.where(lane == 0, inv_hi, jnp.where(lane == 1, inv - inv_hi, 0.0))
            scaled = jnp.concatenate([scaled, extra.astype(BF16)], axis=1)
        gat[i][pos[d2], pos[d1]] = scaled
        for k in (2, 1, 3):
            mine = gat[i].at[pos[d2], pos[d1]]
            exchange(0, i, mine, mine, at(d1, k))

    row = row_iota(256)
    col = col_iota(256)
    source = (row >> 1) & 15
    expand = hot(source == col_iota(16))
    gather_fact = hot(((row_iota(64) & 15) << 4) + (row_iota(64) >> 4) == col)

    def facts_of(j):
        d3 = DIMS[j][2]
        packed = dot(gather_fact, mt2[j].reshape(256, 128)).astype(BF16)
        here = sum(pos[d] * STRIDE[d] for d in range(3) if d != d3)
        expert = here + (row >> 6) * STRIDE[d3] + ((row >> 5) & 1) * 4
        ident, slot = dot(expand, packed[0:16]), dot(expand, packed[16:32])
        match = (ident == expert.astype(F32)) & (slot == (row & 1).astype(F32))
        return packed, match

    def build_select(j):
        tok_of_lane = hot(row_iota(128) & 15 == col & 15)
        match = facts_of(j)[1]
        sel[j] = jnp.where(source == col >> 4, dot(hot(match), tok_of_lane), 0.0).astype(BF16)

    def build_weights(j):
        lane_token = hot(col_iota(128) & 15 == row & 15)
        packed, match = facts_of(j)
        for n, ref in ((2, whi), (3, wlo)):
            val = jnp.where(match, dot(expand, packed[16 * n : 16 * n + 16]), 0.0).astype(BF16)
            spread_out = dot_nt(lane_token, val)
            ref[j] = jnp.where((col >> 1) & 15 == row >> 4, spread_out, 0.0).astype(BF16)

    def build_order(j):
        order_in[j - 1] = hot(slot_index(*coords(row, 0), j) == col)
        order_out[j - 1] = hot(slot_index(*coords(row, j), 0) == col)

    for j in range(3):
        remote(mt2.at[j, pl.ds(0, 3)], mt2.at[j, pl.ds(0, 3)], m2_s.at[j], m2_r.at[j], me).wait_recv()
    for j in range(3):
        build_select(j)
    for j in (1, 2):
        build_order(j)

    for i, (lo, n, j) in enumerate(CHUNKS):
        d1, d2, d3 = DIMS[j]
        arrived(0, i, gat[i].at[0], 3)
        for k in (2, 1, 3):
            mine = gat[i].at[pos[d2]]
            exchange(1, i, mine, mine, at(d2, k))
    for i, (lo, n, j) in enumerate(CHUNKS):
        d1, d2, d3 = DIMS[j]
        arrived(1, i, gat[i], 3)
        rows = dot(sel[j], gat[i][...].reshape(256, WIDTHS[i])).astype(BF16)
        sx[i][...] = rows.reshape(8, 32, WIDTHS[i])
        to_line(2, i, d3, sx[i], ox[i])

    for j in range(3):
        build_weights(j)

    eg_load.wait()
    for i, (lo, n, j) in enumerate(CHUNKS):
        arrived(2, i, ox[i], 7)
        rows = ox[i][...].reshape(256, WIDTHS[i])
        if j != 0:
            rows = dot(order_in[j - 1], rows).astype(BF16)
        part = dot(rows[:, :n], eg[lo : lo + n, :])
        if i == 0:
            hacc[...] = part
        elif i < n_chunk - 1:
            hacc[...] += part
        else:
            inv = rows[:, n : n + 1].astype(F32) + rows[:, n + 1 : n + 2].astype(F32)
            v = (hacc[...] + part) * inv
            hb[0] = (v / (1.0 + jnp.exp(-v))).astype(BF16)
    ed_load.wait()
    for i, (lo, n, j) in enumerate(BACK):
        if i < 3 and j != 0:
            hb[j] = dot(order_out[j - 1], hb[0]).astype(BF16)
        rows = dot(hb[j], ed[:, lo : lo + n]).astype(BF16)
        yx[i][...] = rows.reshape(8, 32, n)
        to_line(3, i, DIMS[j][2], yx[i], qx[i])

    for i, (lo, n, j) in enumerate(BACK):
        d1, d2, d3 = DIMS[j]
        arrived(3, i, qx[i], 7)
        rows = qx[i][...].reshape(256, n)
        summed = (dot(whi[j], rows) + dot(wlo[j], rows)).astype(BF16)
        px[i][...] = summed.reshape(4, 64, n)
        for k in (2, 1, 3):
            exchange(4, i, px[i].at[(pos[d2] + k) % 4], ux[i].at[pos[d2]], at(d2, k))
        ux[i][pos[d2]] = px[i][pos[d2]]
    for i, (lo, n, j) in enumerate(BACK):
        d1, d2, d3 = DIMS[j]
        arrived(4, i, ux[i], 3)
        acc = ux[i][0].astype(F32)
        for q in range(1, 4):
            acc = acc + ux[i][q].astype(F32)
        tx[i][...] = acc.astype(BF16).reshape(4, TOK, n)
        for k in (2, 1, 3):
            exchange(5, i, tx[i].at[(pos[d1] + k) % 4], vx[i].at[pos[d1]], at(d1, k))
        vx[i][pos[d1]] = tx[i][pos[d1]]
    for i, (lo, n, j) in enumerate(BACK):
        arrived(5, i, vx[i], 3)
        acc = hid[:, lo : lo + n].astype(F32)
        for q in range(4):
            acc = acc + vx[i][q].astype(F32)
        out[:, lo : lo + n] = acc.astype(BF16)

    for g in range(groups):
        for k in (1, 2, 3):
            lat_copy(g, k).wait_send()
    for i, (lo, n, j) in enumerate(CHUNKS):
        left = ps.at[pl.ds(0, 3), :, pl.ds(lo, n)]
        remote(left, left, rs_s.at[i], rs_r.at[i], me).wait_send()
    for d in range(3):
        remote(mt1.at[d, pl.ds(0, 3)], mt1.at[d, pl.ds(0, 3)], m1_s.at[d], m1_r.at[d], me).wait_send()
        remote(mt2.at[d, pl.ds(0, 3)], mt2.at[d, pl.ds(0, 3)], m2_s.at[d], m2_r.at[d], me).wait_send()
    def left(ph_no, i, ref, n):
        part = ref.at[pl.ds(0, n)]
        remote(part, part, ex_s.at[ph_no, i], ex_r.at[ph_no, i], me).wait_send()

    for i in range(n_chunk):
        left(0, i, gat[i].at[0], 3)
        left(1, i, gat[i], 3)
        left(2, i, sx[i], 7)
    for i in range(n_back):
        left(3, i, yx[i], 7)
        left(4, i, px[i], 3)
        left(5, i, tx[i], 3)


def per_device(
    hidden_in,
    query_latent,
    query_rope,
    cache_latent,
    cache_rope,
    lengths,
    value_up,
    out_proj,
    norm_gain,
    expert_gate,
    expert_down,
    expert_ids,
    affinity,
):
    n_chunk = len(CHUNKS)
    n_back = len(BACK)
    dma = pltpu.SemaphoreType.DMA
    v = pltpu.VMEM
    scratch = [
        v((TOK, D), BF16),
        v((TOK, HEADS, LAT), BF16),
        v((TOK, HEADS * ROPE), BF16),
        v((HEADS // 2, TOK, 2 * ROPE), BF16),
        v((TOK, CTX, LAT), BF16),
        v((TOK, ROPE, CTX), BF16),
        v((LAT, UPW), BF16),
        v((UPW, D), BF16),
        v((D,), F32),
        v((D, FF), BF16),
        v((FF, D), BF16),
        v((TOPK, TOK), jnp.int32),
        v((TOPK, TOK), F32),
        v((4, TOK, HLOC, LAT), BF16),
        v((4, TOK, HLOC, LAT), BF16),
        v((4, TOK, D), BF16),
        v((4, TOK, D), BF16),
        v((3, 256, FF), BF16),
        v((256, FF), F32),
        v((3, 4, 16, 128), BF16),
        v((3, 4, 4, 16, 128), BF16),
        v((3, 256, 256), BF16),
        v((3, 256, 256), BF16),
        v((3, 256, 256), BF16),
        v((2, 256, 256), BF16),
        v((2, 256, 256), BF16),
    ]
    for shape in ((4, 4, TOK), (8, 32), (8, 32)):
        scratch += [v(shape + (n,), BF16) for n in WIDTHS]
    for shape in ((8, 32), (8, 32), (4, 64), (4, 64), (4, TOK), (4, TOK)):
        scratch += [v(shape + (n,), BF16) for _, n, _ in BACK]
    scratch += [
        dma((3 + 3 * (TOK // GROUP) + 6,)),
        dma((TOK // GROUP, 4)),
        dma((TOK // GROUP, 4)),
        dma((n_chunk,)),
        dma((n_chunk,)),
        dma((3,)),
        dma((3,)),
        dma((3,)),
        dma((3,)),
        dma((6, max(n_chunk, n_back))),
        dma((6, max(n_chunk, n_back))),
    ]
    anyspace = pl.BlockSpec(memory_space=pl.ANY)
    return pl.pallas_call(
        layer_kernel,
        out_shape=pltpu.VMEM((TOK, D), BF16),
        in_specs=[pl.BlockSpec(memory_space=pltpu.SMEM)] + [anyspace] * 12,
        out_specs=pl.BlockSpec(memory_space=pltpu.VMEM),
        scratch_shapes=scratch,
        compiler_params=pltpu.CompilerParams(
            collective_id=0, has_side_effects=True, vmem_limit_bytes=62 * 1024 * 1024
        ),
        name="layer",
    )(
        lengths,
        hidden_in,
        query_latent,
        query_rope,
        cache_latent,
        cache_rope,
        value_up,
        out_proj,
        norm_gain,
        expert_gate,
        expert_down,
        expert_ids.T,
        affinity.T,
    )


def solution(mesh):
    return jax.shard_map(
        per_device,
        mesh=mesh,
        in_specs=(
            P(("dp", "tp"), None),
            P(("dp", "tp"), None, None),
            P(("dp", "tp"), None),
            P(("dp", "tp"), None, None),
            P(("dp", "tp"), None, None),
            P(("dp", "tp")),
            P(None, "tp"),
            P("tp", None),
            P(),
            P(("dp", "tp"), None, None),
            P(("dp", "tp"), None, None),
            P(("dp", "tp"), None),
            P(("dp", "tp"), None),
        ),
        out_specs=P(("dp", "tp"), None),
        check_vma=False,
    )
```
